128 devices in a mesh: tp: 16 (over x_lo, z, core), seq: 8 (over y, x_hi).
Axes of the slice: x: 4 (x_hi: 2, x_lo: 2; x = x_hi * 2 + x_lo), y: 4, z: 4, core: 2. Of those that a mesh axis runs over, the one named last changes fastest.
Arguments:
- residual: bfloat16 [2048, 4096], P('seq'), may hold values from -6 to 6
- mix_gain: float32 [4096], replicated, may hold values from 0.5 to 1.5
- in_proj: bfloat16 [4096, 4096], P(None, 'tp'), may hold values from -0.09375 to 0.09375
- branch_proj: bfloat16 [4096, 4096], P(None, 'tp'), may hold values from -0.09375 to 0.09375
- conv_weight: float32 [4, 4096], P(None, 'tp'), may hold values from -3 to 3
- conv_bias: float32 [4096], P('tp'), may hold values from -1.25 to 1.25
- input_gate: bfloat16 [16, 256, 256], P('tp'), may hold values from -0.375 to 0.375
- input_bias: float32 [4096], P('tp'), may hold values from -3 to 3
- decay_gate: bfloat16 [16, 256, 256], P('tp'), may hold values from -0.375 to 0.375
- decay_bias: float32 [4096], P('tp'), may hold values from -3 to 3
- decay_param: float32 [4096], P('tp'), may hold values from -13 to -2, as said below
- out_proj: bfloat16 [4096, 4096], P('tp'), may hold values from -0.25 to 0.25
- mlp_gain: float32 [4096], replicated, may hold values from 0.5 to 1.5
- gate_proj: bfloat16 [4096, 12288], P('seq', 'tp'), may hold values from -0.09375 to 0.09375
- up_proj: bfloat16 [4096, 12288], P('seq', 'tp'), may hold values from -0.09375 to 0.09375
- down_proj: bfloat16 [12288, 4096], P('tp'), may hold values from -0.078125 to 0.078125
Outputs:
- updated: bfloat16 [2048, 4096], P('seq')
The draws below stay inside these ranges and needn't reach their ends.
Inputs may be any that keep to these rules, and one draw needn't show every extreme that they name: softplus(decay_param) lies between 0.02 / 2048 and 0.1 for every channel.
All inputs are finite; a program needn't handle non-finite values.
Results may differ from the reference program's by a relative error of at most 0.02.
Values may be sent and summed in bfloat16 or wider, within the bound.
A program may use at most 128 MiB of HBM per device.

```python
import jax
import jax.numpy as jnp
from jax import lax

D = 4096
LRU = 4096
FF = 12288
HEADS = 16
CONV = 4
HEAD = 256
TOKENS = 2048


def draw_decay_param(key, part):
    lowest = 0.02 / TOKENS
    highest = 0.1
    spread = jax.random.uniform(key, (LRU,), jnp.float32)
    rate = lowest * jnp.exp(spread * jnp.log(highest / lowest))
    return jnp.log(jnp.expm1(rate)).astype(jnp.float32)


def raised(values, rng, source, target, shards_of, factor):
    owner, partner = [(jnp.arange(values.shape[axis_at]) // (values.shape[axis_at] // shards_of)).reshape([-1 if axis == axis_at else 1 for axis in range(values.ndim)]) for axis_at in (source, target)]
    chosen = jax.random.permutation(rng, shards_of)[partner]
    strong = (owner == chosen) | (owner == (partner + shards_of // 2) % shards_of)
    return jnp.where(strong, factor * values, values)


def steps_of(own_key, shape, shards, low, top_value):
    level = 1.0
    for axis_at, shards_of in shards:
        heights = jax.random.uniform(jax.random.fold_in(jax.random.fold_in(own_key, 6), axis_at), (shards_of,), jnp.float32, low / len(shards), top_value / len(shards))
        level = level * jnp.repeat(jnp.exp(heights), shape[axis_at] // shards_of).reshape((-1,) + (1,) * (len(shape) - 1 - axis_at))
    return level


def scatter_about(own_key, dims, deviation, bound, shards=(), dtype=jnp.bfloat16):
    values = jax.random.normal(own_key, dims, jnp.float32) * deviation
    if len(shards) > 0:
        values = steps_of(own_key, dims, shards, -0.22, 0.18) * values
    return jnp.clip(values, min=-bound, max=bound).astype(dtype)


def noise_with(own_key, extent, scale, most, cuts, heavy, dtype=jnp.bfloat16):
    drawn = scale * jax.random.normal(own_key, extent, jnp.float32)
    if cuts:
        drawn = drawn * steps_of(own_key, extent, cuts, -0.22, 0.18)
    return jnp.clip(raised(drawn, jax.random.fold_in(own_key, 3), *heavy), -most, most).astype(dtype)


def setup_inputs(seed: int = 0) -> dict:
    seeds = jax.random.split(jax.random.key(seed), 17)
    residual = scatter_about(seeds[0], (TOKENS, D), 1.0, 6.0, ((0, 8),))
    mix_gain = jnp.clip(1.0 + 0.1 * jax.random.normal(seeds[1], (D,), jnp.float32), 0.5, 1.5)
    in_proj = scatter_about(seeds[2], (D, LRU), D ** -0.5, 0.09375, ((1, 16),))
    branch_proj = scatter_about(seeds[3], (D, LRU), D ** -0.5, 0.09375, ((1, 16),))
    conv_weight = scatter_about(seeds[4], (CONV, LRU), CONV ** -0.5, 3.0, ((1, 16),), jnp.float32)
    conv_bias = scatter_about(seeds[5], (LRU,), 0.2, 1.25, ((0, 16),), jnp.float32)
    input_gate = scatter_about(seeds[6], (HEADS, HEAD, HEAD), HEAD ** -0.5, 0.375, ((0, 16),))
    input_bias = scatter_about(seeds[7], (LRU,), 0.5, 3.0, ((0, 16),), jnp.float32)
    decay_gate = scatter_about(seeds[8], (HEADS, HEAD, HEAD), HEAD ** -0.5, 0.375, ((0, 16),))
    decay_bias = scatter_about(seeds[9], (LRU,), 0.5, 3.0, ((0, 16),), jnp.float32)
    decay_param = draw_decay_param(jax.random.fold_in(seeds[16], 71), 0)
    out_proj = noise_with(seeds[11], (LRU, D), (LRU // 4) ** -0.5, 0.25, ((0, 16),), (0, 1, 16, 2.0))
    mlp_gain = jnp.clip(1.0 + 0.1 * jax.random.normal(seeds[12], (D,), jnp.float32), 0.5, 1.5)
    gate_proj = scatter_about(seeds[13], (D, FF), D ** -0.5, 0.09375, ((0, 8), (1, 16)))
    up_proj = scatter_about(seeds[14], (D, FF), D ** -0.5, 0.09375, ((0, 8), (1, 16)))
    down_proj = noise_with(seeds[15], (FF, D), FF ** -0.5, 0.078125, ((0, 16),), (0, 1, 16, 2.0))
    return {"residual": residual, "mix_gain": mix_gain, "in_proj": in_proj, "branch_proj": branch_proj, "conv_weight": conv_weight, "conv_bias": conv_bias, "input_gate": input_gate, "input_bias": input_bias, "decay_gate": decay_gate, "decay_bias": decay_bias, "decay_param": decay_param, "out_proj": out_proj, "mlp_gain": mlp_gain, "gate_proj": gate_proj, "up_proj": up_proj, "down_proj": down_proj}


epsilon = 1e-06

def rms_norm(values, gain):
    wide = values.astype(jnp.float32)
    factor = lax.rsqrt(lax.optimization_barrier(jnp.mean(wide * wide, axis=-1, keepdims=True)) + epsilon)
    return (wide * factor * gain).astype(jnp.bfloat16)

def block_gates(values, weight, bias):
    heads, width = (weight.shape[0], weight.shape[1])
    grouped = values.reshape(values.shape[0], heads, width).astype(jnp.float32)
    mixed = jnp.einsum('thi,hij->thj', grouped, weight.astype(jnp.float32))
    return jax.nn.sigmoid(mixed.reshape(values.shape[0], heads * width) + bias)

def smooth(inner, tail, conv_weight, conv_bias):
    taps = conv_weight.shape[0]
    length = inner.shape[0]
    padded = jnp.concatenate([tail, inner], axis=0).astype(jnp.float32)
    total = conv_bias + jnp.zeros((length, inner.shape[1]), jnp.float32)
    for offset in range(taps):
        total = total + conv_weight[offset] * padded[taps - 1 - offset:taps - 1 - offset + length]
    return lax.optimization_barrier(total.astype(jnp.bfloat16))

def advance(state, pair):
    state = pair[0] * state + pair[1]
    return (state, state)

def reference(residual, mix_gain, in_proj, branch_proj, conv_weight, conv_bias, input_gate, input_bias, decay_gate, decay_bias, decay_param, out_proj, mlp_gain, gate_proj, up_proj, down_proj):
    taps = conv_weight.shape[0]
    normed = rms_norm(residual, mix_gain)
    branch = jax.nn.gelu(jnp.dot(normed, branch_proj, preferred_element_type=jnp.float32), approximate=True)
    inner = jnp.dot(normed, in_proj, preferred_element_type=jnp.float32).astype(jnp.bfloat16)
    tail = jnp.zeros((taps - 1, inner.shape[1]), jnp.bfloat16)
    smoothed = smooth(inner, tail, conv_weight, conv_bias)
    input_rate = block_gates(smoothed, input_gate, input_bias)
    decay_rate = block_gates(smoothed, decay_gate, decay_bias)
    log_decay = -8.0 * decay_rate * jax.nn.softplus(decay_param)
    decay = jnp.exp(log_decay)
    first = (jnp.arange(TOKENS) == 0)[:, None]
    scale_in = jnp.where(first, 1.0, jnp.sqrt(-jnp.expm1(2.0 * log_decay)))
    pushed = smoothed.astype(jnp.float32) * input_rate * scale_in
    _, states = lax.scan(advance, jnp.zeros((LRU,), jnp.float32), (decay, pushed))
    gated = (states * branch).astype(jnp.bfloat16)
    mixed = jnp.dot(gated, out_proj, preferred_element_type=jnp.float32)
    middle = lax.optimization_barrier((residual.astype(jnp.float32) + mixed).astype(jnp.bfloat16))
    hidden_in = rms_norm(middle, mlp_gain)
    gate = jnp.dot(hidden_in, gate_proj, preferred_element_type=jnp.float32)
    up = jnp.dot(hidden_in, up_proj, preferred_element_type=jnp.float32)
    hidden = (jax.nn.gelu(gate, approximate=True) * up).astype(jnp.bfloat16)
    output = jnp.dot(hidden, down_proj, preferred_element_type=jnp.float32)
    return (middle.astype(jnp.float32) + output).astype(jnp.bfloat16)
```

```python
import functools
from types import SimpleNamespace

import jax
import jax.numpy as jnp
from jax import lax
from jax.experimental import pallas as pl
from jax.experimental.pallas import tpu as pltpu
from jax.sharding import PartitionSpec as P

epsilon = 1e-06
LOGICAL = pl.DeviceIdType.MESH
LANES = 128
EDGE = 16


def one_minus_exp(x):
    series = 1.0 + x * (1.0 / 9.0)
    for k in range(8, 1, -1):
        series = 1.0 + x * (1.0 / k) * series
    return jnp.where(x > -0.5, -x * series, 1.0 - jnp.exp(x))


def recurrence_phase(
    count,
    taps,
    me,
    tp,
    inner_ref,
    branch_ref,
    conv_weight_ref,
    conv_bias_ref,
    input_gate_ref,
    input_bias_ref,
    decay_gate_ref,
    decay_bias_ref,
    slope_ref,
    gated_ref,
    tail_ref,
    decays_ref,
    states_ref,
    ends_ref,
    arrived_ref,
    tail_send,
    tail_recv,
    end_send,
    end_recv,
):
    length, channels = inner_ref.shape
    heads, head = input_gate_ref.shape[0], input_gate_ref.shape[1]
    peers = [lax.rem(me + offset, count) for offset in range(1, count)]
    tail_copy = remote(
        inner_ref.at[pl.ds(length - EDGE, EDGE), :], tail_ref, tail_send, tail_recv, tp, peers[0]
    )
    tail_copy.start()
    tail_copy.wait()
    follows = jnp.where(me > 0, 1.0, 0.0)

    for h in range(heads):
        columns = pl.ds(h * head, head)
        row = lax.broadcasted_iota(jnp.int32, (length, head), 0)
        current = inner_ref[:, columns].astype(jnp.float32)
        tail = tail_ref[:, columns].astype(jnp.float32) * follows
        before = jnp.concatenate([tail, jnp.zeros((length - EDGE, head), jnp.float32)], axis=0)
        total = conv_bias_ref[:, columns] + conv_weight_ref[0:1, columns] * current
        for tap in range(1, taps):
            shifted = jnp.where(
                row < tap,
                pltpu.roll(before, length + tap - EDGE, 0),
                pltpu.roll(current, tap, 0),
            )
            total = total + conv_weight_ref[tap : tap + 1, columns] * shifted
        smoothed = total.astype(jnp.bfloat16)
        input_rate = jax.nn.sigmoid(
            jnp.dot(smoothed, input_gate_ref[h], preferred_element_type=jnp.float32)
            + input_bias_ref[:, columns]
        )
        decay_rate = jax.nn.sigmoid(
            jnp.dot(smoothed, decay_gate_ref[h], preferred_element_type=jnp.float32)
            + decay_bias_ref[:, columns]
        )
        log_decay = decay_rate * slope_ref[:, columns]
        scale_in = jnp.sqrt(one_minus_exp(2.0 * log_decay))
        scale_in = jnp.where(jnp.logical_and(row == 0, me == 0), 1.0, scale_in)
        decays_ref[:, columns] = jnp.exp(log_decay)
        states_ref[:, columns] = smoothed.astype(jnp.float32) * input_rate * scale_in

    for c in range(channels // LANES):
        columns = pl.ds(c * LANES, LANES)
        row = lax.broadcasted_iota(jnp.int32, (length, LANES), 0)
        decay, state = decays_ref[:, columns], states_ref[:, columns]
        step = 1
        while step < length:
            reached = row >= step
            state = state + decay * jnp.where(reached, pltpu.roll(state, step, 0), 0.0)
            decay = decay * jnp.where(reached, pltpu.roll(decay, step, 0), 1.0)
            step *= 2
        decays_ref[:, columns] = decay
        states_ref[:, columns] = state
        ends_ref[0:1, columns] = decay[length - 1 :, :]
        ends_ref[1:2, columns] = state[length - 1 :, :]

    copies = [
        remote(ends_ref, arrived_ref.at[k], end_send.at[k], end_recv.at[k], tp, peers[k])
        for k in range(count - 1)
    ]
    for copy in copies:
        copy.start()
    for copy in copies:
        copy.wait()
    carried = jnp.zeros((1, channels), jnp.float32)
    for k in range(count - 2, -1, -1):
        new = arrived_ref[k, 0:1, :] * carried + arrived_ref[k, 1:2, :]
        carried = jnp.where(me >= k + 1, new, carried)
    gated_ref[...] = (
        (states_ref[...] + decays_ref[...] * carried) * branch_ref[...]
    ).astype(jnp.bfloat16)


def remote(source, target, send, recv, tp, seq):
    return pltpu.make_async_remote_copy(
        src_ref=source,
        dst_ref=target,
        send_sem=send,
        recv_sem=recv,
        device_id={"tp": tp, "seq": seq},
        device_id_type=LOGICAL,
    )


def aligned(index, unit):
    return pl.multiple_of(index * unit, unit)


class Links:
    def __init__(self):
        self.t, self.s = lax.axis_index("tp"), lax.axis_index("seq")
        self.core = lax.rem(self.t, 2)
        self.z = lax.rem(lax.div(self.t, 2), 4)
        self.xl = lax.div(self.t, 8)
        self.xh = lax.rem(self.s, 2)
        self.y = lax.div(self.s, 2)
        t, s, y, z, core = self.t, self.s, self.y, self.z, self.core
        x = 2 * self.xh + self.xl

        def along_z(step):
            return (8 * self.xl + 2 * lax.rem(z + step, 4) + core, s)

        def along_y(step):
            return (t, 2 * lax.rem(y + step, 4) + self.xh)

        def along_x(step):
            other = lax.rem(x + step, 4)
            return (8 * lax.rem(other, 2) + 2 * z + core, 2 * y + lax.div(other, 2))

        self.pair = (t + 1 - 2 * core, s)
        self.z_up, self.z_down = along_z(1), along_z(3)
        self.y_up, self.y_down = along_y(1), along_y(3)
        self.x_up, self.x_down = along_x(1), along_x(3)
        self.near = (8 * (1 - self.xl) + 2 * z + core, s)
        self.far = (t, 2 * y + 1 - self.xh)
        self.outside = (8 * (1 - self.xl) + 2 * z + core, lax.select(self.xl == 0, self.x_down[1], self.x_up[1]))
        self.sent = []

    def start(self, source, target, send, recv, device):
        copy = remote(source, target, send, recv, *device)
        copy.start()
        self.sent.append(copy)

    def arrived(self, target, send, recv):
        remote(target, target, send, recv, *self.pair).wait_recv()

    def drain(self):
        for copy in self.sent:
            copy.wait_send()
        self.sent = []


GROUPS = 2


def scatter_scratch(length, width):
    bf = jnp.bfloat16
    rows, unit = length // 8, length // 16
    quarter = width // (2 * GROUPS)
    dma = pltpu.SemaphoreType.DMA
    return dict(
        pair=pltpu.VMEM((4, rows, width), bf),
        out_far=pltpu.VMEM((rows, width), bf),
        out_up=pltpu.VMEM((rows, width), bf),
        out_down=pltpu.VMEM((rows, width), bf),
        far_up=pltpu.VMEM((GROUPS, rows, quarter), bf),
        far_down=pltpu.VMEM((GROUPS, rows, quarter), bf),
        from_down=pltpu.VMEM((2 * GROUPS, rows, quarter), bf),
        from_up=pltpu.VMEM((2 * GROUPS, rows, quarter), bf),
        out_near=pltpu.VMEM((unit, width), bf),
        from_near=pltpu.VMEM((GROUPS, unit, 2 * quarter), bf),
        own=pltpu.VMEM((unit, width), jnp.float32),
        pair_s=dma((4, GROUPS)),
        pair_r=dma((4, GROUPS)),
        far_up_s=dma((GROUPS,)),
        far_up_r=dma((GROUPS,)),
        far_down_s=dma((GROUPS,)),
        far_down_r=dma((GROUPS,)),
        up_s=dma((2 * GROUPS,)),
        up_r=dma((2 * GROUPS,)),
        down_s=dma((2 * GROUPS,)),
        down_r=dma((2 * GROUPS,)),
        near_s=dma((GROUPS,)),
        near_r=dma((GROUPS,)),
    )


def owned_row(links, core, z, xl, unit):
    return aligned(core * 8 + z * 2 + xl, unit)


def pair_up(links, part, b, g):
    rows = b.pair.shape[1]
    width = part.shape[1] // GROUPS
    columns = pl.ds(g * width, width)
    for k, step in enumerate((2, 1, 3, 0)):
        block = (1 - links.core) * 4 + lax.rem(links.z + step, 4)
        links.start(
            part.at[pl.ds(aligned(block, rows), rows), columns],
            b.pair.at[k, :, columns],
            b.pair_s.at[k, g],
            b.pair_r.at[k, g],
            links.pair,
        )


def reduce_scatter(links, part, b, finish):
    rows, width = b.pair.shape[1:]
    unit, quarter = rows // 2, width // (2 * GROUPS)
    order = (2, 1, 3, 0)
    starts = [aligned(links.core * 4 + lax.rem(links.z + step, 4), rows) for step in order]

    def summed(k, q):
        columns = pl.ds(q * quarter, quarter)
        return part[pl.ds(starts[k], rows), columns].astype(jnp.float32) + b.pair[
            k, :, columns
        ].astype(jnp.float32)

    def paired(k, g):
        columns = pl.ds(g * 2 * quarter, 2 * quarter)
        links.arrived(b.pair.at[k, :, columns], b.pair_s.at[k, g], b.pair_r.at[k, g])

    def send_far(g):
        paired(0, g)
        for q, landing, send, recv, device in (
            (2 * g, b.far_up, b.far_up_s, b.far_up_r, links.z_up),
            (2 * g + 1, b.far_down, b.far_down_s, b.far_down_r, links.z_down),
        ):
            columns = pl.ds(q * quarter, quarter)
            b.out_far[:, columns] = summed(0, q).astype(jnp.bfloat16)
            links.start(b.out_far.at[:, columns], landing.at[g], send.at[g], recv.at[g], device)

    def send_up(q, value):
        columns = pl.ds(q * quarter, quarter)
        b.out_up[:, columns] = value.astype(jnp.bfloat16)
        links.start(
            b.out_up.at[:, columns], b.from_down.at[q], b.up_s.at[q], b.up_r.at[q], links.z_up
        )

    def send_down(q, value):
        columns = pl.ds(q * quarter, quarter)
        b.out_down[:, columns] = value.astype(jnp.bfloat16)
        links.start(
            b.out_down.at[:, columns], b.from_up.at[q], b.down_s.at[q], b.down_r.at[q], links.z_down
        )

    def send_first(g):
        paired(1, g)
        send_up(2 * g + 1, summed(1, 2 * g + 1))
        paired(2, g)
        send_down(2 * g, summed(2, 2 * g))

    def send_second(g):
        links.arrived(b.far_up.at[g], b.far_up_s.at[g], b.far_up_r.at[g])
        send_up(2 * g, summed(1, 2 * g) + b.far_up[g].astype(jnp.float32))
        links.arrived(b.far_down.at[g], b.far_down_s.at[g], b.far_down_r.at[g])
        send_down(2 * g + 1, summed(2, 2 * g + 1) + b.far_down[g].astype(jnp.float32))

    def collect(g):
        paired(3, g)
        for q in (2 * g, 2 * g + 1):
            links.arrived(b.from_down.at[q], b.up_s.at[q], b.up_r.at[q])
            links.arrived(b.from_up.at[q], b.down_s.at[q], b.down_r.at[q])
            columns = pl.ds(q * quarter, quarter)
            total = (
                summed(3, q)
                + b.from_down[q].astype(jnp.float32)
                + b.from_up[q].astype(jnp.float32)
            )
            low, high = total[:unit], total[unit:]
            first = links.xl == 0
            b.own[:, columns] = jnp.where(first, low, high)
            b.out_near[:, columns] = jnp.where(first, high, low).astype(jnp.bfloat16)
        columns = pl.ds(g * 2 * quarter, 2 * quarter)
        links.start(
            b.out_near.at[:, columns],
            b.from_near.at[g],
            b.near_s.at[g],
            b.near_r.at[g],
            links.near,
        )

    for g in range(GROUPS):
        send_far(g)
        if g == 0:
            send_first(0)
    for g in range(GROUPS):
        send_second(g)
        if g + 1 < GROUPS:
            send_first(g + 1)
    for g in range(GROUPS):
        collect(g)
    for g in range(GROUPS):
        links.arrived(b.from_near.at[g], b.near_s.at[g], b.near_r.at[g])
        columns = pl.ds(g * 2 * quarter, 2 * quarter)
        finish(columns, b.own[:, columns] + b.from_near[g].astype(jnp.float32))


def gather_scratch():
    dma = pltpu.SemaphoreType.DMA
    return dict(
        near_s=dma((2,)),
        near_r=dma((2,)),
        up_s=dma((2, 2)),
        up_r=dma((2, 2)),
        down_s=dma((2, 2)),
        down_r=dma((2, 2)),
        far_up_s=dma((2, 2)),
        far_up_r=dma((2, 2)),
        far_down_s=dma((2, 2)),
        far_down_r=dma((2, 2)),
        pair_s=dma((2, 10)),
        pair_r=dma((2, 10)),
    )


def all_gather(links, slot, unit, b, ready):
    core, z, xl = links.core, links.z, links.xl

    def row(step, i, c=core):
        across = xl if i == 0 else 1 - xl
        return owned_row(links, c, lax.rem(z + step, 4), across, unit)

    def pass_on(h, n, r, half):
        piece = slot(h, r, half)
        links.start(piece, piece, b.pair_s.at[h, n], b.pair_r.at[h, n], links.pair)

    def send(h, i, r):
        piece = slot(h, r, None)
        links.start(piece, piece, b.up_s.at[h, i], b.up_r.at[h, i], links.z_up)
        links.start(piece, piece, b.down_s.at[h, i], b.down_r.at[h, i], links.z_down)

    for h in range(2):
        ready(h)
        own = row(0, 0)
        piece = slot(h, own, None)
        links.start(piece, piece, b.near_s.at[h], b.near_r.at[h], links.near)
        send(h, 0, own)
        pass_on(h, 0, own, None)
    for h in range(2):
        r = row(0, 1)
        links.arrived(slot(h, r, None), b.near_s.at[h], b.near_r.at[h])
        send(h, 1, r)
        pass_on(h, 1, r, None)
    for i in range(2):
        for h in range(2):
            r = row(3, i)
            links.arrived(slot(h, r, None), b.up_s.at[h, i], b.up_r.at[h, i])
            piece = slot(h, r, 0)
            links.start(piece, piece, b.far_up_s.at[h, i], b.far_up_r.at[h, i], links.z_up)
            pass_on(h, 2 + i, r, None)
            r = row(1, i)
            links.arrived(slot(h, r, None), b.down_s.at[h, i], b.down_r.at[h, i])
            piece = slot(h, r, 1)
            links.start(piece, piece, b.far_down_s.at[h, i], b.far_down_r.at[h, i], links.z_down)
            pass_on(h, 4 + i, r, None)
    for i in range(2):
        for h in range(2):
            r = row(2, i)
            links.arrived(slot(h, r, 0), b.far_up_s.at[h, i], b.far_up_r.at[h, i])
            pass_on(h, 6 + i, r, 0)
            links.arrived(slot(h, r, 1), b.far_down_s.at[h, i], b.far_down_r.at[h, i])
            pass_on(h, 8 + i, r, 1)
    for n, (step, i, half) in enumerate(
        [(0, 0, None), (0, 1, None), (3, 0, None), (3, 1, None), (1, 0, None), (1, 1, None)]
        + [(2, 0, 0), (2, 1, 0), (2, 0, 1), (2, 1, 1)]
    ):
        for h in range(2):
            links.arrived(slot(h, row(step, i, 1 - core), half), b.pair_s.at[h, n], b.pair_r.at[h, n])


PIECE = 256


def layer_kernel(
    count,
    taps,
    inner_ref,
    branch_ref,
    conv_weight_ref,
    conv_bias_ref,
    input_gate_ref,
    input_bias_ref,
    decay_gate_ref,
    decay_bias_ref,
    slope_ref,
    gain_ref,
    residual_ref,
    out_proj_ref,
    gate_proj_ref,
    up_proj_ref,
    down_proj_ref,
    out_ref,
    w,
    first,
    second,
    spread,
    final,
):
    w, first, second, spread, final = (SimpleNamespace(**s) for s in (w, first, second, spread, final))
    links = Links()
    length, width = residual_ref.shape
    depth, hidden_width = gate_proj_ref.shape
    unit = length // 16
    half = width // 2
    everyone = [(links.t, lax.rem(links.s + k, count)) for k in range(1, count)]
    everyone += [links.pair, links.z_up, links.z_down, links.near, links.outside]
    barrier = pltpu.get_barrier_semaphore()
    for tp, seq in everyone:
        pl.semaphore_signal(barrier, inc=1, device_id={"tp": tp, "seq": seq}, device_id_type=LOGICAL)
    own = owned_row(links, links.core, links.z, links.xl, unit)
    depth_of = lambda step: pl.ds(aligned(lax.rem(links.y + step, 4), depth), depth)
    loads = [
        pltpu.make_async_copy(out_proj_ref, w.out_proj, w.load.at[0]),
        pltpu.make_async_copy(residual_ref.at[pl.ds(own, unit), :], w.middle, w.load.at[1]),
        pltpu.make_async_copy(gate_proj_ref, w.gate.at[depth_of(0), :], w.load.at[2]),
        pltpu.make_async_copy(up_proj_ref, w.up.at[depth_of(0), :], w.load.at[3]),
        pltpu.make_async_copy(down_proj_ref, w.down, w.load.at[4]),
    ]
    for load in loads:
        load.start()
    pl.semaphore_wait(barrier, len(everyone))

    mine = depth_of(0)
    for target, source, device, at in (
        (w.gate, gate_proj_ref, links.y_up, 0),
        (w.up, up_proj_ref, links.y_down, 1),
        (w.up, up_proj_ref, links.y_up, 2),
        (w.gate, gate_proj_ref, links.y_down, 3),
    ):
        links.start(source, target.at[mine, :], w.gather_s.at[at], w.gather_r.at[at], device)

    recurrence_phase(
        count,
        taps,
        links.s,
        links.t,
        inner_ref,
        branch_ref,
        conv_weight_ref,
        conv_bias_ref,
        input_gate_ref,
        input_bias_ref,
        decay_gate_ref,
        decay_bias_ref,
        slope_ref,
        w.gated,
        w.tail,
        w.decays,
        w.states,
        w.ends,
        w.arrived,
        w.tail_s,
        w.tail_r,
        w.end_s,
        w.end_r,
    )

    def product(left_ref, right_ref, part_ref, scratch):
        tile = 512
        for g in range(GROUPS):

            def step(i, carry):
                columns = pl.ds(aligned(i, tile), tile)
                part_ref[:, columns] = jnp.dot(
                    left_ref[...], right_ref[:, columns], preferred_element_type=jnp.float32
                ).astype(jnp.bfloat16)
                return carry

            steps = width // (GROUPS * tile)
            lax.fori_loop(g * steps, (g + 1) * steps, step, 0)
            pair_up(links, part_ref, scratch, g)

    loads[0].wait()
    product(w.gated, w.out_proj, w.part, first)
    loads[1].wait()

    def to_middle(columns, total):
        w.middle[:, columns] = (total + w.middle[:, columns].astype(jnp.float32)).astype(jnp.bfloat16)

    reduce_scatter(links, w.part, first, to_middle)

    wide = w.middle[...].astype(jnp.float32)
    factor = lax.rsqrt(jnp.mean(wide * wide, axis=-1, keepdims=True) + epsilon)
    w.normed[...] = (wide * factor * gain_ref[...]).astype(jnp.bfloat16)
    hidden_in = w.hidden_in
    for block in range(4):
        place = pl.ds(block * depth, depth)
        there = pl.ds(aligned(2 * block + 1 - links.xh, depth), depth)
        w.away[:, place] = w.normed[:, there]
    links.start(
        w.away, hidden_in.at[links.xh, pl.ds(own, unit), :], w.far_s.at[0], w.far_r.at[0], links.far
    )
    for block in range(4):
        place = pl.ds(block * depth, depth)
        here = pl.ds(aligned(2 * block + links.xh, depth), depth)
        hidden_in[links.xh, pl.ds(own, unit), place] = w.normed[:, here]

    behind, ahead = depth_of(3), depth_of(1)
    links.arrived(w.gate.at[behind, :], w.gather_s.at[0], w.gather_r.at[0])
    piece = w.gate.at[behind, :]
    links.start(piece, piece, w.gather_s.at[4], w.gather_r.at[4], links.y_up)
    links.arrived(w.up.at[ahead, :], w.gather_s.at[1], w.gather_r.at[1])
    piece = w.up.at[ahead, :]
    links.start(piece, piece, w.gather_s.at[5], w.gather_r.at[5], links.y_down)

    def slot(h, r, side):
        group = links.xh if h == 0 else 1 - links.xh
        columns = pl.ds(0, half) if side is None else pl.ds(side * (half // 2), half // 2)
        return hidden_in.at[group, pl.ds(r, unit), columns]

    def ready(h):
        if h == 1:
            links.arrived(slot(1, own, None), w.far_s.at[0], w.far_r.at[0])

    all_gather(links, slot, unit, spread, ready)

    loads[2].wait()
    loads[3].wait()
    links.arrived(w.up.at[behind, :], w.gather_s.at[2], w.gather_r.at[2])
    links.arrived(w.gate.at[ahead, :], w.gather_s.at[3], w.gather_r.at[3])
    opposite = depth_of(2)
    links.arrived(w.gate.at[opposite, :], w.gather_s.at[4], w.gather_r.at[4])
    links.arrived(w.up.at[opposite, :], w.gather_s.at[5], w.gather_r.at[5])

    pieces = hidden_width // PIECE
    top = length // 2
    sides = ((links.x_up, 0), (links.x_down, 1))
    for j in range(pieces):
        columns = pl.ds(j * PIECE, PIECE)
        left = hidden_in[1 - links.xh]
        for n, weights in enumerate((w.gate, w.up)):
            w.given[j, :, n * PIECE : (n + 1) * PIECE] = jnp.dot(
                left, weights[:, columns], preferred_element_type=jnp.float32
            ).astype(jnp.bfloat16)
        for device, d in sides:
            links.start(
                w.given.at[j, pl.ds(d * top, top), :],
                w.relay.at[d, j],
                w.relay_s.at[d, j],
                w.relay_r.at[d, j],
                device,
            )
    for j in range(pieces):
        columns = pl.ds(j * PIECE, PIECE)
        left = hidden_in[links.xh]
        for n, weights in enumerate((w.gate, w.up)):
            w.kept[j, :, n * PIECE : (n + 1) * PIECE] = jnp.dot(
                left, weights[:, columns], preferred_element_type=jnp.float32
            )
    for j in range(pieces):
        for device, d in sides:
            links.arrived(w.relay.at[d, j], w.relay_s.at[d, j], w.relay_r.at[d, j])
            links.start(
                w.relay.at[d, j], w.taken.at[d, j], w.taken_s.at[d, j], w.taken_r.at[d, j], device
            )
    for j in range(pieces):
        for device, d in sides:
            links.arrived(w.taken.at[d, j], w.taken_s.at[d, j], w.taken_r.at[d, j])
            rows = pl.ds(d * top, top)
            both = w.kept[j, rows, :] + w.taken[d, j].astype(jnp.float32)
            w.hidden[rows, j * PIECE : (j + 1) * PIECE] = (
                jax.nn.gelu(both[:, :PIECE], approximate=True) * both[:, PIECE:]
            ).astype(jnp.bfloat16)

    loads[4].wait()
    product(w.hidden, w.down, w.part2, second)

    def to_out(columns, total):
        out_ref[pl.ds(own, unit), columns] = (
            total + w.middle[:, columns].astype(jnp.float32)
        ).astype(jnp.bfloat16)

    reduce_scatter(links, w.part2, second, to_out)

    def place(h, r, side):
        size = half if side is None else half // 2
        return out_ref.at[pl.ds(r, unit), pl.ds(h * half + (0 if side is None else side * size), size)]

    all_gather(links, place, unit, final, lambda h: None)
    links.drain()


def layer(
    inner,
    branch,
    conv_weight,
    conv_bias,
    input_gate,
    input_bias,
    decay_gate,
    decay_bias,
    slope,
    gain,
    residual,
    out_proj,
    gate_proj,
    up_proj,
    down_proj,
):
    count = lax.axis_size("seq")
    length, channels = inner.shape
    width = residual.shape[1]
    depth, hidden_width = gate_proj.shape
    unit = length // 16
    bf, f32 = jnp.bfloat16, jnp.float32
    dma = pltpu.SemaphoreType.DMA
    vmem = pl.BlockSpec(memory_space=pltpu.VMEM)
    anywhere = pl.BlockSpec(memory_space=pl.ANY)
    pieces = hidden_width // PIECE
    scratch = dict(
        out_proj=pltpu.VMEM(out_proj.shape, bf),
        middle=pltpu.VMEM((unit, width), bf),
        normed=pltpu.VMEM((unit, width), bf),
        away=pltpu.VMEM((unit, width // 2), bf),
        gate=pltpu.VMEM((4 * depth, hidden_width), bf),
        up=pltpu.VMEM((4 * depth, hidden_width), bf),
        down=pltpu.VMEM(down_proj.shape, bf),
        hidden_in=pltpu.VMEM((2, length, width // 2), bf),
        given=pltpu.VMEM((pieces, length, 2 * PIECE), bf),
        kept=pltpu.VMEM((pieces, length, 2 * PIECE), f32),
        relay=pltpu.VMEM((2, pieces, length // 2, 2 * PIECE), bf),
        taken=pltpu.VMEM((2, pieces, length // 2, 2 * PIECE), bf),
        hidden=pltpu.VMEM((length, hidden_width), bf),
        part=pltpu.VMEM((length, width), bf),
        part2=pltpu.VMEM((length, width), bf),
        gated=pltpu.VMEM((length, channels), bf),
        tail=pltpu.VMEM((EDGE, channels), bf),
        decays=pltpu.VMEM((length, channels), f32),
        states=pltpu.VMEM((length, channels), f32),
        ends=pltpu.VMEM((8, channels), f32),
        arrived=pltpu.VMEM((count - 1, 8, channels), f32),
        tail_s=dma,
        tail_r=dma,
        end_s=dma((count - 1,)),
        end_r=dma((count - 1,)),
        load=dma((5,)),
        gather_s=dma((6,)),
        gather_r=dma((6,)),
        far_s=dma((1,)),
        far_r=dma((1,)),
        relay_s=dma((2, pieces)),
        relay_r=dma((2, pieces)),
        taken_s=dma((2, pieces)),
        taken_r=dma((2, pieces)),
    )
    return pl.pallas_call(
        functools.partial(layer_kernel, count, conv_weight.shape[0]),
        out_shape=jax.ShapeDtypeStruct((length, width), bf),
        in_specs=[vmem] * 10 + [anywhere] * 5,
        out_specs=vmem,
        scratch_shapes=(
            scratch,
            scatter_scratch(length, width),
            scatter_scratch(length, width),
            gather_scratch(),
            gather_scratch(),
        ),
        compiler_params=pltpu.CompilerParams(
            collective_id=0, has_side_effects=True, vmem_limit_bytes=56 * 2**20
        ),
    )(
        inner,
        branch,
        conv_weight,
        conv_bias[None],
        input_gate,
        input_bias[None],
        decay_gate,
        decay_bias[None],
        slope[None],
        gain[None],
        residual,
        out_proj,
        gate_proj,
        up_proj,
        down_proj,
    )


def rms_norm(values, gain):
    wide = values.astype(jnp.float32)
    factor = lax.rsqrt(jnp.mean(wide * wide, axis=-1, keepdims=True) + epsilon)
    return (wide * factor * gain).astype(jnp.bfloat16)


def on_device(
    residual,
    mix_gain,
    in_proj,
    branch_proj,
    conv_weight,
    conv_bias,
    input_gate,
    input_bias,
    decay_gate,
    decay_bias,
    decay_param,
    out_proj,
    mlp_gain,
    gate_proj,
    up_proj,
    down_proj,
):
    normed = rms_norm(residual, mix_gain)
    branch = jax.nn.gelu(
        jnp.dot(normed, branch_proj, preferred_element_type=jnp.float32), approximate=True
    )
    inner = jnp.dot(normed, in_proj, preferred_element_type=jnp.float32).astype(jnp.bfloat16)
    return layer(
        inner,
        branch,
        conv_weight,
        conv_bias,
        input_gate,
        input_bias,
        decay_gate,
        decay_bias,
        -8.0 * jax.nn.softplus(decay_param),
        mlp_gain,
        residual,
        out_proj,
        gate_proj,
        up_proj,
        down_proj,
    )


def solution(mesh):
    in_specs = (
        P("seq", None),
        P(),
        P(None, "tp"),
        P(None, "tp"),
        P(None, "tp"),
        P("tp"),
        P("tp", None, None),
        P("tp"),
        P("tp", None, None),
        P("tp"),
        P("tp"),
        P("tp", None),
        P(),
        P("seq", "tp"),
        P("seq", "tp"),
        P("tp", None),
    )
    out_specs = P("seq", None)
    return jax.shard_map(
        on_device, mesh=mesh, in_specs=in_specs, out_specs=out_specs, check_vma=False
    )
```

```python
import functools
from types import SimpleNamespace

import jax
import jax.numpy as jnp
from jax import lax
from jax.experimental import pallas as pl
from jax.experimental.pallas import tpu as pltpu
from jax.sharding import PartitionSpec as P

epsilon = 1e-06
LOGICAL = pl.DeviceIdType.MESH
LANES = 128
EDGE = 8
GRANT = 44 * 2**20


def one_minus_exp(x):
    series = 1.0 + x * (1.0 / 9.0)
    for k in range(8, 1, -1):
        series = 1.0 + x * (1.0 / k) * series
    return jnp.where(x > -0.5, -x * series, 1.0 - jnp.exp(x))


def softplus(v):
    small = jnp.exp(-jnp.abs(v))
    whole = 1.0 + small
    grown = jnp.where(whole == 1.0, small, jnp.log(whole) * small / jnp.where(whole == 1.0, 1.0, whole - 1.0))
    return jnp.maximum(v, 0.0) + grown


def local_states(
    taps,
    me,
    inner_ref,
    conv_weight_ref,
    conv_bias_ref,
    input_gate_ref,
    input_bias_ref,
    decay_gate_ref,
    decay_bias_ref,
    decay_param_ref,
    decays_ref,
    states_ref,
    ends_ref,
):
    length, channels = inner_ref.shape[0] - EDGE, inner_ref.shape[1]
    heads, head = input_gate_ref.shape[0], input_gate_ref.shape[1]
    follows = jnp.where(me > 0, 1.0, 0.0)

    for h in range(heads):
        columns = pl.ds(h * head, head)
        row = lax.broadcasted_iota(jnp.int32, (length, head), 0)
        current = inner_ref[:length, columns].astype(jnp.float32)
        tail = inner_ref[length:, columns].astype(jnp.float32) * follows
        before = jnp.concatenate([tail, jnp.zeros((length - EDGE, head), jnp.float32)], axis=0)
        total = conv_bias_ref[:, columns] + conv_weight_ref[0:1, columns] * current
        for tap in range(1, taps):
            shifted = jnp.where(
                row < tap,
                pltpu.roll(before, length + tap - EDGE, 0),
                pltpu.roll(current, tap, 0),
            )
            total = total + conv_weight_ref[tap : tap + 1, columns] * shifted
        smoothed = total.astype(jnp.bfloat16)
        input_rate = jax.nn.sigmoid(
            jnp.dot(smoothed, input_gate_ref[h], preferred_element_type=jnp.float32)
            + input_bias_ref[:, columns]
        )
        decay_rate = jax.nn.sigmoid(
            jnp.dot(smoothed, decay_gate_ref[h], preferred_element_type=jnp.float32)
            + decay_bias_ref[:, columns]
        )
        log_decay = decay_rate * (-8.0 * softplus(decay_param_ref[:, columns]))
        scale_in = jnp.sqrt(one_minus_exp(2.0 * log_decay))
        scale_in = jnp.where(jnp.logical_and(row == 0, me == 0), 1.0, scale_in)
        decays_ref[:, columns] = jnp.exp(log_decay)
        states_ref[:, columns] = smoothed.astype(jnp.float32) * input_rate * scale_in

    for c in range(channels // LANES):
        columns = pl.ds(c * LANES, LANES)
        row = lax.broadcasted_iota(jnp.int32, (length, LANES), 0)
        decay, state = decays_ref[:, columns], states_ref[:, columns]
        step = 1
        while step < length:
            reached = row >= step
            state = state + decay * jnp.where(reached, pltpu.roll(state, step, 0), 0.0)
            decay = decay * jnp.where(reached, pltpu.roll(decay, step, 0), 1.0)
            step *= 2
        decays_ref[:, columns] = decay
        states_ref[:, columns] = state
        ends_ref[0:1, columns] = decay[length - 1 :, :]
        ends_ref[1:2, columns] = state[length - 1 :, :]


def remote(source, target, send, recv, tp, seq):
    return pltpu.make_async_remote_copy(
        src_ref=source,
        dst_ref=target,
        send_sem=send,
        recv_sem=recv,
        device_id={"tp": tp, "seq": seq},
        device_id_type=LOGICAL,
    )


def aligned(index, unit):
    return pl.multiple_of(index * unit, unit)


class Links:
    def __init__(self):
        self.t, self.s = lax.axis_index("tp"), lax.axis_index("seq")
        self.core = lax.rem(self.t, 2)
        self.z = lax.rem(lax.div(self.t, 2), 4)
        self.xl = lax.div(self.t, 8)
        self.xh = lax.rem(self.s, 2)
        self.y = lax.div(self.s, 2)
        t, s, y, z, core = self.t, self.s, self.y, self.z, self.core
        x = 2 * self.xh + self.xl

        def along_z(step):
            return (8 * self.xl + 2 * lax.rem(z + step, 4) + core, s)

        def along_y(step):
            return (t, 2 * lax.rem(y + step, 4) + self.xh)

        def along_x(step):
            other = lax.rem(x + step, 4)
            return (8 * lax.rem(other, 2) + 2 * z + core, 2 * y + lax.div(other, 2))

        self.pair = (t + 1 - 2 * core, s)
        self.z_up, self.z_down = along_z(1), along_z(3)
        self.y_up, self.y_down = along_y(1), along_y(3)
        self.x_up, self.x_down = along_x(1), along_x(3)
        self.near = (8 * (1 - self.xl) + 2 * z + core, s)
        self.far = (t, 2 * y + 1 - self.xh)
        self.outside = (8 * (1 - self.xl) + 2 * z + core, lax.select(self.xl == 0, self.x_down[1], self.x_up[1]))
        self.sent = []

    def start(self, source, target, send, recv, device):
        copy = remote(source, target, send, recv, *device)
        copy.start()
        self.sent.append(copy)

    def arrived(self, target, send, recv):
        remote(target, target, send, recv, *self.pair).wait_recv()

    def drain(self):
        for copy in self.sent:
            copy.wait_send()
        self.sent = []


GROUPS = 2


def scatter_scratch(length, width):
    bf = jnp.bfloat16
    rows, unit = length // 8, length // 16
    quarter = width // (2 * GROUPS)
    dma = pltpu.SemaphoreType.DMA
    return dict(
        pair=pltpu.VMEM((4, rows, width), bf),
        out_far=pltpu.VMEM((rows, width), bf),
        out_up=pltpu.VMEM((rows, width), bf),
        out_down=pltpu.VMEM((rows, width), bf),
        far_up=pltpu.VMEM((GROUPS, rows, quarter), bf),
        far_down=pltpu.VMEM((GROUPS, rows, quarter), bf),
        from_down=pltpu.VMEM((2 * GROUPS, rows, quarter), bf),
        from_up=pltpu.VMEM((2 * GROUPS, rows, quarter), bf),
        out_near=pltpu.VMEM((unit, width), bf),
        from_near=pltpu.VMEM((GROUPS, unit, 2 * quarter), bf),
        own=pltpu.VMEM((unit, width), jnp.float32),
        pair_s=dma((4, GROUPS)),
        pair_r=dma((4, GROUPS)),
        far_up_s=dma((GROUPS,)),
        far_up_r=dma((GROUPS,)),
        far_down_s=dma((GROUPS,)),
        far_down_r=dma((GROUPS,)),
        up_s=dma((2 * GROUPS,)),
        up_r=dma((2 * GROUPS,)),
        down_s=dma((2 * GROUPS,)),
        down_r=dma((2 * GROUPS,)),
        near_s=dma((GROUPS,)),
        near_r=dma((GROUPS,)),
    )


def owned_row(links, core, z, xl, unit):
    return aligned(core * 8 + z * 2 + xl, unit)


def pair_up(links, part, b, g):
    rows = b.pair.shape[1]
    width = part.shape[1] // GROUPS
    columns = pl.ds(g * width, width)
    for k, step in enumerate((2, 1, 3, 0)):
        block = (1 - links.core) * 4 + lax.rem(links.z + step, 4)
        links.start(
            part.at[pl.ds(aligned(block, rows), rows), columns],
            b.pair.at[k, :, columns],
            b.pair_s.at[k, g],
            b.pair_r.at[k, g],
            links.pair,
        )


def reduce_scatter(links, part, b, finish):
    rows, width = b.pair.shape[1:]
    unit, quarter = rows // 2, width // (2 * GROUPS)
    order = (2, 1, 3, 0)
    starts = [aligned(links.core * 4 + lax.rem(links.z + step, 4), rows) for step in order]

    def summed(k, q):
        columns = pl.ds(q * quarter, quarter)
        return part[pl.ds(starts[k], rows), columns].astype(jnp.float32) + b.pair[
            k, :, columns
        ].astype(jnp.float32)

    def paired(k, g):
        columns = pl.ds(g * 2 * quarter, 2 * quarter)
        links.arrived(b.pair.at[k, :, columns], b.pair_s.at[k, g], b.pair_r.at[k, g])

    def send_far(g):
        paired(0, g)
        for q, landing, send, recv, device in (
            (2 * g, b.far_up, b.far_up_s, b.far_up_r, links.z_up),
            (2 * g + 1, b.far_down, b.far_down_s, b.far_down_r, links.z_down),
        ):
            columns = pl.ds(q * quarter, quarter)
            b.out_far[:, columns] = summed(0, q).astype(jnp.bfloat16)
            links.start(b.out_far.at[:, columns], landing.at[g], send.at[g], recv.at[g], device)

    def send_up(q, value):
        columns = pl.ds(q * quarter, quarter)
        b.out_up[:, columns] = value.astype(jnp.bfloat16)
        links.start(
            b.out_up.at[:, columns], b.from_down.at[q], b.up_s.at[q], b.up_r.at[q], links.z_up
        )

    def send_down(q, value):
        columns = pl.ds(q * quarter, quarter)
        b.out_down[:, columns] = value.astype(jnp.bfloat16)
        links.start(
            b.out_down.at[:, columns], b.from_up.at[q], b.down_s.at[q], b.down_r.at[q], links.z_down
        )

    def send_first(g):
        paired(1, g)
        send_up(2 * g + 1, summed(1, 2 * g + 1))
        paired(2, g)
        send_down(2 * g, summed(2, 2 * g))

    def send_second(g):
        links.arrived(b.far_up.at[g], b.far_up_s.at[g], b.far_up_r.at[g])
        send_up(2 * g, summed(1, 2 * g) + b.far_up[g].astype(jnp.float32))
        links.arrived(b.far_down.at[g], b.far_down_s.at[g], b.far_down_r.at[g])
        send_down(2 * g + 1, summed(2, 2 * g + 1) + b.far_down[g].astype(jnp.float32))

    def collect(g):
        paired(3, g)
        for q in (2 * g, 2 * g + 1):
            links.arrived(b.from_down.at[q], b.up_s.at[q], b.up_r.at[q])
            links.arrived(b.from_up.at[q], b.down_s.at[q], b.down_r.at[q])
            columns = pl.ds(q * quarter, quarter)
            total = (
                summed(3, q)
                + b.from_down[q].astype(jnp.float32)
                + b.from_up[q].astype(jnp.float32)
            )
            low, high = total[:unit], total[unit:]
            first = links.xl == 0
            b.own[:, columns] = jnp.where(first, low, high)
            b.out_near[:, columns] = jnp.where(first, high, low).astype(jnp.bfloat16)
        columns = pl.ds(g * 2 * quarter, 2 * quarter)
        links.start(
            b.out_near.at[:, columns],
            b.from_near.at[g],
            b.near_s.at[g],
            b.near_r.at[g],
            links.near,
        )

    for g in range(GROUPS):
        send_far(g)
        if g == 0:
            send_first(0)
    for g in range(GROUPS):
        send_second(g)
        if g + 1 < GROUPS:
            send_first(g + 1)
    for g in range(GROUPS):
        collect(g)
    for g in range(GROUPS):
        links.arrived(b.from_near.at[g], b.near_s.at[g], b.near_r.at[g])
        columns = pl.ds(g * 2 * quarter, 2 * quarter)
        finish(columns, b.own[:, columns] + b.from_near[g].astype(jnp.float32))


def gather_scratch():
    dma = pltpu.SemaphoreType.DMA
    return dict(
        near_s=dma((2,)),
        near_r=dma((2,)),
        up_s=dma((2, 2)),
        up_r=dma((2, 2)),
        down_s=dma((2, 2)),
        down_r=dma((2, 2)),
        far_up_s=dma((2, 2)),
        far_up_r=dma((2, 2)),
        far_down_s=dma((2, 2)),
        far_down_r=dma((2, 2)),
        pair_s=dma((2, 10)),
        pair_r=dma((2, 10)),
    )


def all_gather(links, slot, unit, b, ready):
    core, z, xl = links.core, links.z, links.xl

    def row(step, i, c=core):
        across = xl if i == 0 else 1 - xl
        return owned_row(links, c, lax.rem(z + step, 4), across, unit)

    def pass_on(h, n, r, half):
        piece = slot(h, r, half)
        links.start(piece, piece, b.pair_s.at[h, n], b.pair_r.at[h, n], links.pair)

    def send(h, i, r):
        piece = slot(h, r, None)
        links.start(piece, piece, b.up_s.at[h, i], b.up_r.at[h, i], links.z_up)
        links.start(piece, piece, b.down_s.at[h, i], b.down_r.at[h, i], links.z_down)

    for h in range(2):
        ready(h)
        own = row(0, 0)
        piece = slot(h, own, None)
        links.start(piece, piece, b.near_s.at[h], b.near_r.at[h], links.near)
        send(h, 0, own)
        pass_on(h, 0, own, None)
    for h in range(2):
        r = row(0, 1)
        links.arrived(slot(h, r, None), b.near_s.at[h], b.near_r.at[h])
        send(h, 1, r)
        pass_on(h, 1, r, None)
    for i in range(2):
        for h in range(2):
            r = row(3, i)
            links.arrived(slot(h, r, None), b.up_s.at[h, i], b.up_r.at[h, i])
            piece = slot(h, r, 0)
            links.start(piece, piece, b.far_up_s.at[h, i], b.far_up_r.at[h, i], links.z_up)
            pass_on(h, 2 + i, r, None)
            r = row(1, i)
            links.arrived(slot(h, r, None), b.down_s.at[h, i], b.down_r.at[h, i])
            piece = slot(h, r, 1)
            links.start(piece, piece, b.far_down_s.at[h, i], b.far_down_r.at[h, i], links.z_down)
            pass_on(h, 4 + i, r, None)
    for i in range(2):
        for h in range(2):
            r = row(2, i)
            links.arrived(slot(h, r, 0), b.far_up_s.at[h, i], b.far_up_r.at[h, i])
            pass_on(h, 6 + i, r, 0)
            links.arrived(slot(h, r, 1), b.far_down_s.at[h, i], b.far_down_r.at[h, i])
            pass_on(h, 8 + i, r, 1)
    for n, (step, i, half) in enumerate(
        [(0, 0, None), (0, 1, None), (3, 0, None), (3, 1, None), (1, 0, None), (1, 1, None)]
        + [(2, 0, 0), (2, 1, 0), (2, 0, 1), (2, 1, 1)]
    ):
        for h in range(2):
            links.arrived(slot(h, row(step, i, 1 - core), half), b.pair_s.at[h, n], b.pair_r.at[h, n])


PIECE = 256


CHUNKS = 4


def layer_kernel(
    count,
    taps,
    *refs,
):
    outside, (out_ref, w, first, second, spread, final) = refs[:9], refs[16:]
    residual_ref, in_proj_ref, branch_proj_ref, out_proj_ref, gate_proj_ref, up_proj_ref, down_proj_ref = refs[9:16]
    w, first, second, spread, final = (SimpleNamespace(**s) for s in (w, first, second, spread, final))
    links = Links()
    length, width = residual_ref.shape
    depth, hidden_width = gate_proj_ref.shape
    unit = length // 16
    half = width // 2
    peers = [(links.t, lax.rem(links.s + k, count)) for k in range(1, count)]
    everyone = peers + [links.pair, links.z_up, links.z_down, links.near, links.outside]
    barrier = pltpu.get_barrier_semaphore()
    for tp, seq in everyone:
        pl.semaphore_signal(barrier, inc=1, device_id={"tp": tp, "seq": seq}, device_id_type=LOGICAL)
    own = owned_row(links, links.core, links.z, links.xl, unit)

    behind, here, ahead, opposite = (p * depth for p in range(4))
    loads = [
        pltpu.make_async_copy(residual_ref, w.normed.at[pl.ds(0, length), :], w.load.at[0]),
        pltpu.make_async_copy(in_proj_ref, w.in_proj, w.load.at[1]),
        pltpu.make_async_copy(branch_proj_ref, w.branch_proj, w.load.at[2]),
        pltpu.make_async_copy(out_proj_ref, w.out_proj, w.load.at[3]),
        pltpu.make_async_copy(residual_ref.at[pl.ds(own, unit), :], w.middle, w.load.at[4]),
        pltpu.make_async_copy(gate_proj_ref, w.gate.at[pl.ds(here, depth), :], w.load.at[5]),
        pltpu.make_async_copy(up_proj_ref, w.up.at[pl.ds(here, depth), :], w.load.at[6]),
        pltpu.make_async_copy(down_proj_ref, w.down, w.load.at[7]),
    ]
    small_loads = [
        pltpu.make_async_copy(source, target, w.small_load.at[k])
        for k, (source, target) in enumerate(zip(outside, w.small))
    ]
    for load in loads[:2] + small_loads + loads[2:3]:
        load.start()
    (
        mix_gain_ref,
        conv_weight_ref,
        conv_bias_ref,
        input_gate_ref,
        input_bias_ref,
        decay_gate_ref,
        decay_bias_ref,
        decay_param_ref,
        gain_ref,
    ) = w.small
    pl.semaphore_wait(barrier, len(everyone))

    edge = pl.ds(length, EDGE)
    links.start(
        residual_ref.at[pl.ds(length - EDGE, EDGE), :], w.normed.at[edge, :], w.tail_s, w.tail_r, peers[0]
    )
    share = depth // CHUNKS

    def gather(n):
        rows = pl.ds(n % CHUNKS * share, share)
        sides = ((gate_proj_ref, w.gate), (up_proj_ref, w.up))
        for d, device in enumerate((links.y_up, links.y_down)):
            source, target = sides[(n // CHUNKS + d) % 2]
            there = pl.ds((ahead if d else behind) + n % CHUNKS * share, share)
            links.start(
                source.at[rows, :], target.at[there, :], w.gather_s.at[d, n], w.gather_r.at[d, n], device
            )

    def gathered(d, n):
        target = (w.gate, w.up)[(n // CHUNKS + d) % 2] if n < 2 * CHUNKS else (w.gate, w.up)[d]
        start = (ahead if d else behind) if n < 2 * CHUNKS else opposite
        piece = target.at[pl.ds(start + n % CHUNKS * share, share), :]
        links.arrived(piece, w.gather_s.at[d, n], w.gather_r.at[d, n])
        return target

    def forward(n):
        for d, device in enumerate((links.y_up, links.y_down)):
            target = gathered(d, n)
            source = pl.ds((ahead if d else behind) + n * share, share)
            there = pl.ds(opposite + n * share, share)
            at = 2 * CHUNKS + n
            links.start(
                target.at[source, :], target.at[there, :], w.gather_s.at[d, at], w.gather_r.at[d, at], device
            )

    gather(0)
    for load in loads[3:]:
        load.start()

    def norm(start, rows):
        place = pl.ds(start, rows)
        wide = w.normed[place, :].astype(jnp.float32)
        factor = lax.rsqrt(jnp.mean(wide * wide, axis=-1, keepdims=True) + epsilon)
        w.normed[place, :] = (wide * factor * mix_gain_ref[...]).astype(jnp.bfloat16)

    def norm_step(i, carry):
        norm(aligned(i, unit), unit)
        return carry

    for load in small_loads:
        load.wait()
    loads[0].wait()
    lax.fori_loop(0, 16, norm_step, 0)
    links.arrived(w.normed.at[edge, :], w.tail_s, w.tail_r)
    norm(length, EDGE)
    loads[1].wait()
    w.inner[...] = jnp.dot(w.normed[...], w.in_proj[...], preferred_element_type=jnp.float32).astype(
        jnp.bfloat16
    )
    local_states(
        taps,
        links.s,
        w.inner,
        conv_weight_ref,
        conv_bias_ref,
        input_gate_ref,
        input_bias_ref,
        decay_gate_ref,
        decay_bias_ref,
        decay_param_ref,
        w.decays,
        w.states,
        w.ends,
    )
    for k in range(count - 1):
        links.start(w.ends, w.arrived.at[k], w.end_s.at[k], w.end_r.at[k], peers[k])
    for n in range(1, 2 * CHUNKS):
        gather(n)
    loads[2].wait()
    branch = jax.nn.gelu(
        jnp.dot(w.normed[:length, :], w.branch_proj[...], preferred_element_type=jnp.float32), approximate=True
    )
    carried = jnp.zeros((1, w.ends.shape[1]), jnp.float32)
    for k in range(count - 2, -1, -1):
        links.arrived(w.arrived.at[k], w.end_s.at[k], w.end_r.at[k])
        new = w.arrived[k, 0:1, :] * carried + w.arrived[k, 1:2, :]
        carried = jnp.where(links.s >= k + 1, new, carried)
    w.gated[...] = ((w.states[...] + w.decays[...] * carried) * branch).astype(jnp.bfloat16)

    def product(left_ref, right_ref, part_ref, scratch):
        tile = 512
        for g in range(GROUPS):

            def step(i, carry):
                columns = pl.ds(aligned(i, tile), tile)
                part_ref[:, columns] = jnp.dot(
                    left_ref[...], right_ref[:, columns], preferred_element_type=jnp.float32
                ).astype(jnp.bfloat16)
                return carry

            steps = width // (GROUPS * tile)
            lax.fori_loop(g * steps, (g + 1) * steps, step, 0)
            pair_up(links, part_ref, scratch, g)

    loads[3].wait()
    product(w.gated, w.out_proj, w.part, first)
    loads[4].wait()

    def to_middle(columns, total):
        w.middle[:, columns] = (total + w.middle[:, columns].astype(jnp.float32)).astype(jnp.bfloat16)

    reduce_scatter(links, w.part, first, to_middle)

    wide = w.middle[...].astype(jnp.float32)
    factor = lax.rsqrt(jnp.mean(wide * wide, axis=-1, keepdims=True) + epsilon)
    w.chosen[...] = (wide * factor * gain_ref[...]).astype(jnp.bfloat16)
    hidden_in = w.hidden_in

    def features(p, which):
        return pl.ds(aligned(2 * lax.rem(links.y + 3 + p, 4) + which, depth), depth)

    for p in range(4):
        w.away[:, p * depth : (p + 1) * depth] = w.chosen[:, features(p, 1 - links.xh)]
    links.start(
        w.away, hidden_in.at[links.xh, pl.ds(own, unit), :], w.far_s.at[0], w.far_r.at[0], links.far
    )
    for p in range(4):
        hidden_in[links.xh, pl.ds(own, unit), p * depth : (p + 1) * depth] = w.chosen[:, features(p, links.xh)]
    for n in range(CHUNKS):
        forward(n)

    def slot(h, r, side):
        group = links.xh if h == 0 else 1 - links.xh
        columns = pl.ds(0, half) if side is None else pl.ds(side * (half // 2), half // 2)
        return hidden_in.at[group, pl.ds(r, unit), columns]

    def ready(h):
        if h == 1:
            links.arrived(slot(1, own, None), w.far_s.at[0], w.far_r.at[0])

    all_gather(links, slot, unit, spread, ready)

    loads[5].wait()
    loads[6].wait()
    for n in range(CHUNKS, 2 * CHUNKS):
        for d in range(2):
            gathered(d, n)

    pieces = hidden_width // PIECE
    top = length // 2
    sides = ((links.x_up, 0), (links.x_down, 1))

    def partial(group, j, place):
        return jnp.concatenate(
            [
                jnp.dot(
                    hidden_in[group, :, place],
                    weights[place, j * PIECE : (j + 1) * PIECE],
                    preferred_element_type=jnp.float32,
                )
                for weights in (w.gate, w.up)
            ],
            axis=1,
        )

    nearby, distant = pl.ds(0, opposite), pl.ds(opposite, depth)
    for j in range(pieces):
        w.lent[j] = partial(1 - links.xh, j, nearby)
    for j in range(pieces):
        w.kept[j] = partial(links.xh, j, nearby)
    for n in range(CHUNKS):
        for d in range(2):
            gathered(d, 2 * CHUNKS + n)
    for j in range(pieces):
        w.given[j] = (w.lent[j] + partial(1 - links.xh, j, distant)).astype(jnp.bfloat16)
        for device, d in sides:
            links.start(
                w.given.at[j, pl.ds(d * top, top), :],
                w.relay.at[d, j],
                w.relay_s.at[d, j],
                w.relay_r.at[d, j],
                device,
            )
    for j in range(pieces):
        w.kept[j] += partial(links.xh, j, distant)
    for j in range(pieces):
        for device, d in sides:
            links.arrived(w.relay.at[d, j], w.relay_s.at[d, j], w.relay_r.at[d, j])
            links.start(
                w.relay.at[d, j], w.taken.at[d, j], w.taken_s.at[d, j], w.taken_r.at[d, j], device
            )
    for j in range(pieces):
        for device, d in sides:
            links.arrived(w.taken.at[d, j], w.taken_s.at[d, j], w.taken_r.at[d, j])
            rows = pl.ds(d * top, top)
            both = w.kept[j, rows, :] + w.taken[d, j].astype(jnp.float32)
            w.hidden[rows, j * PIECE : (j + 1) * PIECE] = (
                jax.nn.gelu(both[:, :PIECE], approximate=True) * both[:, PIECE:]
            ).astype(jnp.bfloat16)

    loads[7].wait()
    product(w.hidden, w.down, w.part2, second)

    def to_out(columns, total):
        out_ref[pl.ds(own, unit), columns] = (
            total + w.middle[:, columns].astype(jnp.float32)
        ).astype(jnp.bfloat16)

    reduce_scatter(links, w.part2, second, to_out)

    def place(h, r, side):
        size = half if side is None else half // 2
        return out_ref.at[pl.ds(r, unit), pl.ds(h * half + (0 if side is None else side * size), size)]

    all_gather(links, place, unit, final, lambda h: None)
    links.drain()


def on_device(
    residual,
    mix_gain,
    in_proj,
    branch_proj,
    conv_weight,
    conv_bias,
    input_gate,
    input_bias,
    decay_gate,
    decay_bias,
    decay_param,
    out_proj,
    mlp_gain,
    gate_proj,
    up_proj,
    down_proj,
):
    count = lax.axis_size("seq")
    length, width = residual.shape
    channels = in_proj.shape[1]
    depth, hidden_width = gate_proj.shape
    unit = length // 16
    bf, f32 = jnp.bfloat16, jnp.float32
    dma = pltpu.SemaphoreType.DMA
    outer = pl.BlockSpec(memory_space=pltpu.HBM)
    pieces = hidden_width // PIECE
    small = (
        mix_gain[None],
        conv_weight,
        conv_bias[None],
        input_gate,
        input_bias[None],
        decay_gate,
        decay_bias[None],
        decay_param[None],
        mlp_gain[None],
    )
    scratch = dict(
        small=tuple(pltpu.VMEM(array.shape, array.dtype) for array in small),
        small_load=dma((len(small),)),
        normed=pltpu.VMEM((length + EDGE, width), bf),
        in_proj=pltpu.VMEM(in_proj.shape, bf),
        branch_proj=pltpu.VMEM(branch_proj.shape, bf),
        inner=pltpu.VMEM((length + EDGE, channels), bf),
        out_proj=pltpu.VMEM(out_proj.shape, bf),
        middle=pltpu.VMEM((unit, width), bf),
        chosen=pltpu.VMEM((unit, width), bf),
        away=pltpu.VMEM((unit, width // 2), bf),
        gate=pltpu.VMEM((4 * depth, hidden_width), bf),
        up=pltpu.VMEM((4 * depth, hidden_width), bf),
        down=pltpu.VMEM(down_proj.shape, bf),
        hidden_in=pltpu.VMEM((2, length, width // 2), bf),
        given=pltpu.VMEM((pieces, length, 2 * PIECE), bf),
        lent=pltpu.VMEM((pieces, length, 2 * PIECE), f32),
        kept=pltpu.VMEM((pieces, length, 2 * PIECE), f32),
        relay=pltpu.VMEM((2, pieces, length // 2, 2 * PIECE), bf),
        taken=pltpu.VMEM((2, pieces, length // 2, 2 * PIECE), bf),
        hidden=pltpu.VMEM((length, hidden_width), bf),
        part=pltpu.VMEM((length, width), bf),
        part2=pltpu.VMEM((length, width), bf),
        gated=pltpu.VMEM((length, channels), bf),
        decays=pltpu.VMEM((length, channels), f32),
        states=pltpu.VMEM((length, channels), f32),
        ends=pltpu.VMEM((8, channels), f32),
        arrived=pltpu.VMEM((count - 1, 8, channels), f32),
        tail_s=dma,
        tail_r=dma,
        end_s=dma((count - 1,)),
        end_r=dma((count - 1,)),
        load=dma((8,)),
        gather_s=dma((2, 3 * CHUNKS)),
        gather_r=dma((2, 3 * CHUNKS)),
        far_s=dma((1,)),
        far_r=dma((1,)),
        relay_s=dma((2, pieces)),
        relay_r=dma((2, pieces)),
        taken_s=dma((2, pieces)),
        taken_r=dma((2, pieces)),
    )
    return pl.pallas_call(
        functools.partial(layer_kernel, count, conv_weight.shape[0]),
        out_shape=jax.ShapeDtypeStruct((length, width), bf),
        in_specs=[outer] * 16,
        out_specs=pl.BlockSpec(memory_space=pltpu.VMEM),
        scratch_shapes=(
            scratch,
            scatter_scratch(length, width),
            scatter_scratch(length, width),
            gather_scratch(),
            gather_scratch(),
        ),
        compiler_params=pltpu.CompilerParams(
            collective_id=0, has_side_effects=True, vmem_limit_bytes=GRANT
        ),
    )(
        *(
            pltpu.with_memory_space_constraint(array, pltpu.HBM)
            for array in (
                *small,
                residual,
                in_proj,
                branch_proj,
                out_proj,
                gate_proj,
                up_proj,
                down_proj,
            )
        )
    )


def solution(mesh):
    in_specs = (
        P("seq", None),
        P(),
        P(None, "tp"),
        P(None, "tp"),
        P(None, "tp"),
        P("tp"),
        P("tp", None, None),
        P("tp"),
        P("tp", None, None),
        P("tp"),
        P("tp"),
        P("tp", None),
        P(),
        P("seq", "tp"),
        P("seq", "tp"),
        P("tp", None),
    )
    out_specs = P("seq", None)
    return jax.shard_map(
        on_device, mesh=mesh, in_specs=in_specs, out_specs=out_specs, check_vma=False
    )
```

```python
import functools
from types import SimpleNamespace

import jax
import jax.numpy as jnp
from jax import lax
from jax.experimental import pallas as pl
from jax.experimental.pallas import tpu as pltpu
from jax.sharding import PartitionSpec as P

epsilon = 1e-06
LOGICAL = pl.DeviceIdType.MESH
LANES = 128
EDGE = 8
GRANT = 50 * 2**20


def one_minus_exp(x):
    series = 1.0 + x * (1.0 / 9.0)
    for k in range(8, 1, -1):
        series = 1.0 + x * (1.0 / k) * series
    return jnp.where(x > -0.5, -x * series, 1.0 - jnp.exp(x))


def softplus(v):
    small = jnp.exp(-jnp.abs(v))
    whole = 1.0 + small
    grown = jnp.where(whole == 1.0, small, jnp.log(whole) * small / jnp.where(whole == 1.0, 1.0, whole - 1.0))
    return jnp.maximum(v, 0.0) + grown


def local_states(
    taps,
    me,
    inner_ref,
    conv_weight_ref,
    conv_bias_ref,
    input_gate_ref,
    input_bias_ref,
    decay_gate_ref,
    decay_bias_ref,
    decay_param_ref,
    decays_ref,
    states_ref,
    ends_ref,
):
    length, channels = inner_ref.shape[0] - EDGE, inner_ref.shape[1]
    heads, head = input_gate_ref.shape[0], input_gate_ref.shape[1]
    follows = jnp.where(me > 0, 1.0, 0.0)

    for h in range(heads):
        columns = pl.ds(h * head, head)
        row = lax.broadcasted_iota(jnp.int32, (length, head), 0)
        current = inner_ref[:length, columns].astype(jnp.float32)
        tail = inner_ref[length:, columns].astype(jnp.float32) * follows
        before = jnp.concatenate([tail, jnp.zeros((length - EDGE, head), jnp.float32)], axis=0)
        total = conv_bias_ref[:, columns] + conv_weight_ref[0:1, columns] * current
        for tap in range(1, taps):
            shifted = jnp.where(
                row < tap,
                pltpu.roll(before, length + tap - EDGE, 0),
                pltpu.roll(current, tap, 0),
            )
            total = total + conv_weight_ref[tap : tap + 1, columns] * shifted
        smoothed = total.astype(jnp.bfloat16)
        input_rate = jax.nn.sigmoid(
            jnp.dot(smoothed, input_gate_ref[h], preferred_element_type=jnp.float32)
            + input_bias_ref[:, columns]
        )
        decay_rate = jax.nn.sigmoid(
            jnp.dot(smoothed, decay_gate_ref[h], preferred_element_type=jnp.float32)
            + decay_bias_ref[:, columns]
        )
        log_decay = decay_rate * (-8.0 * softplus(decay_param_ref[:, columns]))
        scale_in = jnp.sqrt(one_minus_exp(2.0 * log_decay))
        scale_in = jnp.where(jnp.logical_and(row == 0, me == 0), 1.0, scale_in)
        decays_ref[:, columns] = jnp.exp(log_decay)
        states_ref[:, columns] = smoothed.astype(jnp.float32) * input_rate * scale_in

    for c in range(channels // LANES):
        columns = pl.ds(c * LANES, LANES)
        row = lax.broadcasted_iota(jnp.int32, (length, LANES), 0)
        decay, state = decays_ref[:, columns], states_ref[:, columns]
        step = 1
        while step < length:
            reached = row >= step
            state = state + decay * jnp.where(reached, pltpu.roll(state, step, 0), 0.0)
            decay = decay * jnp.where(reached, pltpu.roll(decay, step, 0), 1.0)
            step *= 2
        decays_ref[:, columns] = decay
        states_ref[:, columns] = state
        ends_ref[0:1, columns] = decay[length - 1 :, :]
        ends_ref[1:2, columns] = state[length - 1 :, :]


def remote(source, target, send, recv, tp, seq):
    return pltpu.make_async_remote_copy(
        src_ref=source,
        dst_ref=target,
        send_sem=send,
        recv_sem=recv,
        device_id={"tp": tp, "seq": seq},
        device_id_type=LOGICAL,
    )


def aligned(index, unit):
    return pl.multiple_of(index * unit, unit)


class Links:
    def __init__(self):
        self.t, self.s = lax.axis_index("tp"), lax.axis_index("seq")
        self.core = lax.rem(self.t, 2)
        self.z = lax.rem(lax.div(self.t, 2), 4)
        self.xl = lax.div(self.t, 8)
        self.xh = lax.rem(self.s, 2)
        self.y = lax.div(self.s, 2)
        t, s, y, z, core = self.t, self.s, self.y, self.z, self.core
        x = 2 * self.xh + self.xl

        def along_z(step):
            return (8 * self.xl + 2 * lax.rem(z + step, 4) + core, s)

        def along_y(step):
            return (t, 2 * lax.rem(y + step, 4) + self.xh)

        def along_x(step):
            other = lax.rem(x + step, 4)
            return (8 * lax.rem(other, 2) + 2 * z + core, 2 * y + lax.div(other, 2))

        self.pair = (t + 1 - 2 * core, s)
        self.z_up, self.z_down = along_z(1), along_z(3)
        self.y_up, self.y_down = along_y(1), along_y(3)
        self.x_up, self.x_down = along_x(1), along_x(3)
        self.near = (8 * (1 - self.xl) + 2 * z + core, s)
        self.far = (t, 2 * y + 1 - self.xh)
        self.outside = (8 * (1 - self.xl) + 2 * z + core, lax.select(self.xl == 0, self.x_down[1], self.x_up[1]))
        self.sent = []

    def start(self, source, target, send, recv, device):
        copy = remote(source, target, send, recv, *device)
        copy.start()
        self.sent.append(copy)

    def arrived(self, target, send, recv):
        remote(target, target, send, recv, *self.pair).wait_recv()

    def drain(self):
        for copy in self.sent:
            copy.wait_send()
        self.sent = []


GROUPS = 2


def scatter_scratch(length, width):
    bf = jnp.bfloat16
    rows, unit = length // 8, length // 16
    quarter = width // (2 * GROUPS)
    dma = pltpu.SemaphoreType.DMA
    return dict(
        pair=pltpu.VMEM((4, rows, width), bf),
        out_far=pltpu.VMEM((rows, width), bf),
        out_up=pltpu.VMEM((rows, width), bf),
        out_down=pltpu.VMEM((rows, width), bf),
        far_up=pltpu.VMEM((GROUPS, rows, quarter), bf),
        far_down=pltpu.VMEM((GROUPS, rows, quarter), bf),
        from_down=pltpu.VMEM((2 * GROUPS, rows, quarter), bf),
        from_up=pltpu.VMEM((2 * GROUPS, rows, quarter), bf),
        out_near=pltpu.VMEM((unit, width), bf),
        from_near=pltpu.VMEM((GROUPS, unit, 2 * quarter), bf),
        own=pltpu.VMEM((unit, width), jnp.float32),
        pair_s=dma((4, GROUPS)),
        pair_r=dma((4, GROUPS)),
        far_up_s=dma((GROUPS,)),
        far_up_r=dma((GROUPS,)),
        far_down_s=dma((GROUPS,)),
        far_down_r=dma((GROUPS,)),
        up_s=dma((2 * GROUPS,)),
        up_r=dma((2 * GROUPS,)),
        down_s=dma((2 * GROUPS,)),
        down_r=dma((2 * GROUPS,)),
        near_s=dma((GROUPS,)),
        near_r=dma((GROUPS,)),
    )


def owned_row(links, core, z, xl, unit):
    return aligned(core * 8 + z * 2 + xl, unit)


def pair_up(links, part, b, g):
    rows = b.pair.shape[1]
    width = part.shape[1] // GROUPS
    columns = pl.ds(g * width, width)
    for k, step in enumerate((2, 1, 3, 0)):
        block = (1 - links.core) * 4 + lax.rem(links.z + step, 4)
        links.start(
            part.at[pl.ds(aligned(block, rows), rows), columns],
            b.pair.at[k, :, columns],
            b.pair_s.at[k, g],
            b.pair_r.at[k, g],
            links.pair,
        )


def reduce_scatter(links, part, b, finish):
    rows, width = b.pair.shape[1:]
    unit, quarter = rows // 2, width // (2 * GROUPS)
    order = (2, 1, 3, 0)
    starts = [aligned(links.core * 4 + lax.rem(links.z + step, 4), rows) for step in order]

    def summed(k, q):
        columns = pl.ds(q * quarter, quarter)
        return part[pl.ds(starts[k], rows), columns].astype(jnp.float32) + b.pair[
            k, :, columns
        ].astype(jnp.float32)

    def paired(k, g):
        columns = pl.ds(g * 2 * quarter, 2 * quarter)
        links.arrived(b.pair.at[k, :, columns], b.pair_s.at[k, g], b.pair_r.at[k, g])

    def send_far(g):
        paired(0, g)
        for q, landing, send, recv, device in (
            (2 * g, b.far_up, b.far_up_s, b.far_up_r, links.z_up),
            (2 * g + 1, b.far_down, b.far_down_s, b.far_down_r, links.z_down),
        ):
            columns = pl.ds(q * quarter, quarter)
            b.out_far[:, columns] = summed(0, q).astype(jnp.bfloat16)
            links.start(b.out_far.at[:, columns], landing.at[g], send.at[g], recv.at[g], device)

    def send_up(q, value):
        columns = pl.ds(q * quarter, quarter)
        b.out_up[:, columns] = value.astype(jnp.bfloat16)
        links.start(
            b.out_up.at[:, columns], b.from_down.at[q], b.up_s.at[q], b.up_r.at[q], links.z_up
        )

    def send_down(q, value):
        columns = pl.ds(q * quarter, quarter)
        b.out_down[:, columns] = value.astype(jnp.bfloat16)
        links.start(
            b.out_down.at[:, columns], b.from_up.at[q], b.down_s.at[q], b.down_r.at[q], links.z_down
        )

    def send_first(g):
        paired(1, g)
        send_up(2 * g + 1, summed(1, 2 * g + 1))
        paired(2, g)
        send_down(2 * g, summed(2, 2 * g))

    def send_second(g):
        links.arrived(b.far_up.at[g], b.far_up_s.at[g], b.far_up_r.at[g])
        send_up(2 * g, summed(1, 2 * g) + b.far_up[g].astype(jnp.float32))
        links.arrived(b.far_down.at[g], b.far_down_s.at[g], b.far_down_r.at[g])
        send_down(2 * g + 1, summed(2, 2 * g + 1) + b.far_down[g].astype(jnp.float32))

    def collect(g):
        paired(3, g)
        for q in (2 * g, 2 * g + 1):
            links.arrived(b.from_down.at[q], b.up_s.at[q], b.up_r.at[q])
            links.arrived(b.from_up.at[q], b.down_s.at[q], b.down_r.at[q])
            columns = pl.ds(q * quarter, quarter)
            total = (
                summed(3, q)
                + b.from_down[q].astype(jnp.float32)
                + b.from_up[q].astype(jnp.float32)
            )
            low, high = total[:unit], total[unit:]
            first = links.xl == 0
            b.own[:, columns] = jnp.where(first, low, high)
            b.out_near[:, columns] = jnp.where(first, high, low).astype(jnp.bfloat16)
        columns = pl.ds(g * 2 * quarter, 2 * quarter)
        links.start(
            b.out_near.at[:, columns],
            b.from_near.at[g],
            b.near_s.at[g],
            b.near_r.at[g],
            links.near,
        )

    for g in range(GROUPS):
        send_far(g)
        if g == 0:
            send_first(0)
    for g in range(GROUPS):
        send_second(g)
        if g + 1 < GROUPS:
            send_first(g + 1)
    for g in range(GROUPS):
        collect(g)
    for g in range(GROUPS):
        links.arrived(b.from_near.at[g], b.near_s.at[g], b.near_r.at[g])
        columns = pl.ds(g * 2 * quarter, 2 * quarter)
        finish(columns, b.own[:, columns] + b.from_near[g].astype(jnp.float32))


def gather_scratch():
    dma = pltpu.SemaphoreType.DMA
    return dict(
        near_s=dma((2,)),
        near_r=dma((2,)),
        up_s=dma((2, 2)),
        up_r=dma((2, 2)),
        down_s=dma((2, 2)),
        down_r=dma((2, 2)),
        far_up_s=dma((2, 2)),
        far_up_r=dma((2, 2)),
        far_down_s=dma((2, 2)),
        far_down_r=dma((2, 2)),
        pair_s=dma((2, 10)),
        pair_r=dma((2, 10)),
    )


def all_gather(links, slot, unit, b, ready):
    core, z, xl = links.core, links.z, links.xl

    def row(step, i, c=core):
        across = xl if i == 0 else 1 - xl
        return owned_row(links, c, lax.rem(z + step, 4), across, unit)

    def pass_on(h, n, r, half):
        piece = slot(h, r, half)
        links.start(piece, piece, b.pair_s.at[h, n], b.pair_r.at[h, n], links.pair)

    def send(h, i, r):
        piece = slot(h, r, None)
        links.start(piece, piece, b.up_s.at[h, i], b.up_r.at[h, i], links.z_up)
        links.start(piece, piece, b.down_s.at[h, i], b.down_r.at[h, i], links.z_down)

    for h in range(2):
        ready(h)
        own = row(0, 0)
        piece = slot(h, own, None)
        links.start(piece, piece, b.near_s.at[h], b.near_r.at[h], links.near)
        send(h, 0, own)
        pass_on(h, 0, own, None)
    for h in range(2):
        r = row(0, 1)
        links.arrived(slot(h, r, None), b.near_s.at[h], b.near_r.at[h])
        send(h, 1, r)
        pass_on(h, 1, r, None)
    for i in range(2):
        for h in range(2):
            r = row(3, i)
            links.arrived(slot(h, r, None), b.up_s.at[h, i], b.up_r.at[h, i])
            piece = slot(h, r, 0)
            links.start(piece, piece, b.far_up_s.at[h, i], b.far_up_r.at[h, i], links.z_up)
            pass_on(h, 2 + i, r, None)
            r = row(1, i)
            links.arrived(slot(h, r, None), b.down_s.at[h, i], b.down_r.at[h, i])
            piece = slot(h, r, 1)
            links.start(piece, piece, b.far_down_s.at[h, i], b.far_down_r.at[h, i], links.z_down)
            pass_on(h, 4 + i, r, None)
    for i in range(2):
        for h in range(2):
            r = row(2, i)
            links.arrived(slot(h, r, 0), b.far_up_s.at[h, i], b.far_up_r.at[h, i])
            pass_on(h, 6 + i, r, 0)
            links.arrived(slot(h, r, 1), b.far_down_s.at[h, i], b.far_down_r.at[h, i])
            pass_on(h, 8 + i, r, 1)
    for n, (step, i, half) in enumerate(
        [(0, 0, None), (0, 1, None), (3, 0, None), (3, 1, None), (1, 0, None), (1, 1, None)]
        + [(2, 0, 0), (2, 1, 0), (2, 0, 1), (2, 1, 1)]
    ):
        for h in range(2):
            links.arrived(slot(h, row(step, i, 1 - core), half), b.pair_s.at[h, n], b.pair_r.at[h, n])


PIECE = 128


CHUNKS = 4


def layer_kernel(
    count,
    taps,
    *refs,
):
    outside, (out_ref, w, first, second, spread, final) = refs[:9], refs[16:]
    residual_ref, in_proj_ref, branch_proj_ref, out_proj_ref, gate_proj_ref, up_proj_ref, down_proj_ref = refs[9:16]
    w, first, second, spread, final = (SimpleNamespace(**s) for s in (w, first, second, spread, final))
    links = Links()
    length, width = residual_ref.shape
    depth, hidden_width = gate_proj_ref.shape
    unit = length // 16
    half = width // 2
    peers = [(links.t, lax.rem(links.s + k, count)) for k in range(1, count)]
    everyone = peers + [links.pair, links.z_up, links.z_down, links.near, links.outside]
    barrier = pltpu.get_barrier_semaphore()
    for tp, seq in everyone:
        pl.semaphore_signal(barrier, inc=1, device_id={"tp": tp, "seq": seq}, device_id_type=LOGICAL)
    own = owned_row(links, links.core, links.z, links.xl, unit)

    behind, here, ahead, opposite = (p * depth for p in range(4))
    loads = [
        pltpu.make_async_copy(residual_ref, w.normed.at[pl.ds(0, length), :], w.load.at[0]),
        pltpu.make_async_copy(in_proj_ref, w.in_proj, w.load.at[1]),
        pltpu.make_async_copy(branch_proj_ref, w.branch_proj, w.load.at[2]),
        pltpu.make_async_copy(out_proj_ref, w.out_proj, w.load.at[3]),
        pltpu.make_async_copy(residual_ref.at[pl.ds(own, unit), :], w.middle, w.load.at[4]),
        pltpu.make_async_copy(gate_proj_ref, w.gate.at[pl.ds(here, depth), :], w.load.at[5]),
        pltpu.make_async_copy(up_proj_ref, w.up.at[pl.ds(here, depth), :], w.load.at[6]),
        pltpu.make_async_copy(down_proj_ref, w.down, w.load.at[7]),
    ]
    small_loads = [
        pltpu.make_async_copy(source, target, w.small_load.at[k])
        for k, (source, target) in enumerate(zip(outside, w.small))
    ]
    for load in loads[:2] + small_loads + loads[2:3]:
        load.start()
    (
        mix_gain_ref,
        conv_weight_ref,
        conv_bias_ref,
        input_gate_ref,
        input_bias_ref,
        decay_gate_ref,
        decay_bias_ref,
        decay_param_ref,
        gain_ref,
    ) = w.small
    pl.semaphore_wait(barrier, len(everyone))

    edge = pl.ds(length, EDGE)
    links.start(
        residual_ref.at[pl.ds(length - EDGE, EDGE), :], w.normed.at[edge, :], w.tail_s, w.tail_r, peers[0]
    )
    share = depth // CHUNKS

    def gather(n):
        rows = pl.ds(n % CHUNKS * share, share)
        sides = ((gate_proj_ref, w.gate), (up_proj_ref, w.up))
        for d, device in enumerate((links.y_up, links.y_down)):
            source, target = sides[(n // CHUNKS + d) % 2]
            there = pl.ds((ahead if d else behind) + n % CHUNKS * share, share)
            links.start(
                source.at[rows, :], target.at[there, :], w.gather_s.at[d, n], w.gather_r.at[d, n], device
            )

    def gathered(d, n):
        target = (w.gate, w.up)[(n // CHUNKS + d) % 2]
        piece = target.at[pl.ds((ahead if d else behind) + n % CHUNKS * share, share), :]
        links.arrived(piece, w.gather_s.at[d, n], w.gather_r.at[d, n])

    pieces = hidden_width // PIECE
    onward = ((links.y_up, w.gate, behind), (links.y_down, w.up, ahead))

    def forward(j):
        columns = pl.ds(j * PIECE, PIECE)
        for d, (device, target, start) in enumerate(onward):
            links.start(
                target.at[pl.ds(start, depth), columns],
                target.at[pl.ds(opposite, depth), columns],
                w.forward_s.at[d, j],
                w.forward_r.at[d, j],
                device,
            )

    def forwarded(j):
        columns = pl.ds(j * PIECE, PIECE)
        for d, (device, target, start) in enumerate(onward):
            links.arrived(target.at[pl.ds(opposite, depth), columns], w.forward_s.at[d, j], w.forward_r.at[d, j])

    gather(0)
    for load in loads[3:]:
        load.start()

    def norm(start, rows):
        place = pl.ds(start, rows)
        wide = w.normed[place, :].astype(jnp.float32)
        factor = lax.rsqrt(jnp.mean(wide * wide, axis=-1, keepdims=True) + epsilon)
        w.normed[place, :] = (wide * factor * mix_gain_ref[...]).astype(jnp.bfloat16)

    def norm_step(i, carry):
        norm(aligned(i, unit), unit)
        return carry

    for load in small_loads:
        load.wait()
    loads[0].wait()
    lax.fori_loop(0, 16, norm_step, 0)
    links.arrived(w.normed.at[edge, :], w.tail_s, w.tail_r)
    norm(length, EDGE)
    loads[1].wait()
    w.inner[...] = jnp.dot(w.normed[...], w.in_proj[...], preferred_element_type=jnp.float32).astype(
        jnp.bfloat16
    )
    local_states(
        taps,
        links.s,
        w.inner,
        conv_weight_ref,
        conv_bias_ref,
        input_gate_ref,
        input_bias_ref,
        decay_gate_ref,
        decay_bias_ref,
        decay_param_ref,
        w.decays,
        w.states,
        w.ends,
    )
    for k in range(count - 1):
        links.start(w.ends, w.arrived.at[k], w.end_s.at[k], w.end_r.at[k], peers[k])
    for n in range(1, 2 * CHUNKS):
        gather(n)
    loads[2].wait()
    branch = jax.nn.gelu(
        jnp.dot(w.normed[:length, :], w.branch_proj[...], preferred_element_type=jnp.float32), approximate=True
    )
    carried = jnp.zeros((1, w.ends.shape[1]), jnp.float32)
    for k in range(count - 2, -1, -1):
        links.arrived(w.arrived.at[k], w.end_s.at[k], w.end_r.at[k])
        new = w.arrived[k, 0:1, :] * carried + w.arrived[k, 1:2, :]
        carried = jnp.where(links.s >= k + 1, new, carried)
    w.gated[...] = ((w.states[...] + w.decays[...] * carried) * branch).astype(jnp.bfloat16)

    def product(left_ref, right_ref, part_ref, scratch, total_ref=None):
        tile = 512
        for g in range(GROUPS):

            def step(i, carry):
                columns = pl.ds(aligned(i, tile), tile)
                value = jnp.dot(left_ref[...], right_ref[:, columns], preferred_element_type=jnp.float32)
                if total_ref is not None:
                    value = value + total_ref[:, columns]
                part_ref[:, columns] = value.astype(jnp.bfloat16)
                return carry

            steps = width // (GROUPS * tile)
            lax.fori_loop(g * steps, (g + 1) * steps, step, 0)
            pair_up(links, part_ref, scratch, g)

    loads[3].wait()
    product(w.gated, w.out_proj, w.part, first)
    loads[4].wait()

    def to_middle(columns, total):
        w.middle[:, columns] = (total + w.middle[:, columns].astype(jnp.float32)).astype(jnp.bfloat16)

    reduce_scatter(links, w.part, first, to_middle)

    wide = w.middle[...].astype(jnp.float32)
    factor = lax.rsqrt(jnp.mean(wide * wide, axis=-1, keepdims=True) + epsilon)
    w.chosen[...] = (wide * factor * gain_ref[...]).astype(jnp.bfloat16)
    hidden_in = w.hidden_in

    def features(p, which):
        return pl.ds(aligned(2 * lax.rem(links.y + 3 + p, 4) + which, depth), depth)

    for p in range(4):
        w.away[:, p * depth : (p + 1) * depth] = w.chosen[:, features(p, 1 - links.xh)]
    links.start(
        w.away, hidden_in.at[links.xh, pl.ds(own, unit), :], w.far_s.at[0], w.far_r.at[0], links.far
    )
    for p in range(4):
        hidden_in[links.xh, pl.ds(own, unit), p * depth : (p + 1) * depth] = w.chosen[:, features(p, links.xh)]
    for n in range(CHUNKS):
        for d in range(2):
            gathered(d, n)
    for j in range(pieces):
        forward(j)

    def slot(h, r, side):
        group = links.xh if h == 0 else 1 - links.xh
        columns = pl.ds(0, half) if side is None else pl.ds(side * (half // 2), half // 2)
        return hidden_in.at[group, pl.ds(r, unit), columns]

    def ready(h):
        if h == 1:
            links.arrived(slot(1, own, None), w.far_s.at[0], w.far_r.at[0])

    all_gather(links, slot, unit, spread, ready)

    loads[5].wait()
    loads[6].wait()
    for n in range(CHUNKS, 2 * CHUNKS):
        for d in range(2):
            gathered(d, n)

    top = length // 2
    sides = ((links.x_up, 0), (links.x_down, 1))

    def partial(group, j, place):
        return jnp.concatenate(
            [
                jnp.dot(
                    hidden_in[group, :, place],
                    weights[place, j * PIECE : (j + 1) * PIECE],
                    preferred_element_type=jnp.float32,
                )
                for weights in (w.gate, w.up)
            ],
            axis=1,
        )

    nearby, distant = pl.ds(0, opposite), pl.ds(opposite, depth)
    for j in range(pieces):
        w.lent[j] = partial(1 - links.xh, j, nearby)
    for j in range(pieces):
        w.kept[j] = partial(links.xh, j, nearby)
    def give(j):
        forwarded(j)
        w.given[j] = (w.lent[j] + partial(1 - links.xh, j, distant)).astype(jnp.bfloat16)
        for device, d in sides:
            links.start(
                w.given.at[j, pl.ds(d * top, top), :],
                w.relay.at[d, j],
                w.relay_s.at[d, j],
                w.relay_r.at[d, j],
                device,
            )

    def keep(j):
        w.kept[j] += partial(links.xh, j, distant)

    def pass_on(j):
        for device, d in sides:
            links.arrived(w.relay.at[d, j], w.relay_s.at[d, j], w.relay_r.at[d, j])
            links.start(
                w.relay.at[d, j], w.taken.at[d, j], w.taken_s.at[d, j], w.taken_r.at[d, j], device
            )

    def take(j):
        for device, d in sides:
            links.arrived(w.taken.at[d, j], w.taken_s.at[d, j], w.taken_r.at[d, j])
            rows = pl.ds(d * top, top)
            both = w.kept[j, rows, :] + w.taken[d, j].astype(jnp.float32)
            w.hidden[rows, j * PIECE : (j + 1) * PIECE] = (
                jax.nn.gelu(both[:, :PIECE], approximate=True) * both[:, PIECE:]
            ).astype(jnp.bfloat16)

    for j in range(pieces):
        give(j)
        if j > 0:
            pass_on(j - 1)
        keep(j)
        if j > 2:
            take(j - 3)
    pass_on(pieces - 1)
    take(pieces - 3)

    loads[7].wait()
    early = (pieces - 2) * PIECE

    def sum_early(i, carry):
        columns = pl.ds(aligned(i, 512), 512)
        w.total[:, columns] = jnp.dot(
            w.hidden[:, :early], w.down[:early, columns], preferred_element_type=jnp.float32
        )
        return carry

    lax.fori_loop(0, width // 512, sum_early, 0)
    take(pieces - 2)
    take(pieces - 1)
    product(w.hidden.at[:, pl.ds(early, 2 * PIECE)], w.down.at[pl.ds(early, 2 * PIECE), :], w.part2, second, w.total)

    def to_out(columns, total):
        out_ref[pl.ds(own, unit), columns] = (
            total + w.middle[:, columns].astype(jnp.float32)
        ).astype(jnp.bfloat16)

    reduce_scatter(links, w.part2, second, to_out)

    def place(h, r, side):
        size = half if side is None else half // 2
        return out_ref.at[pl.ds(r, unit), pl.ds(h * half + (0 if side is None else side * size), size)]

    all_gather(links, place, unit, final, lambda h: None)
    links.drain()


def on_device(
    residual,
    mix_gain,
    in_proj,
    branch_proj,
    conv_weight,
    conv_bias,
    input_gate,
    input_bias,
    decay_gate,
    decay_bias,
    decay_param,
    out_proj,
    mlp_gain,
    gate_proj,
    up_proj,
    down_proj,
):
    count = lax.axis_size("seq")
    length, width = residual.shape
    channels = in_proj.shape[1]
    depth, hidden_width = gate_proj.shape
    unit = length // 16
    bf, f32 = jnp.bfloat16, jnp.float32
    dma = pltpu.SemaphoreType.DMA
    outer = pl.BlockSpec(memory_space=pltpu.HBM)
    pieces = hidden_width // PIECE
    small = (
        mix_gain[None],
        conv_weight,
        conv_bias[None],
        input_gate,
        input_bias[None],
        decay_gate,
        decay_bias[None],
        decay_param[None],
        mlp_gain[None],
    )
    scratch = dict(
        small=tuple(pltpu.VMEM(array.shape, array.dtype) for array in small),
        small_load=dma((len(small),)),
        normed=pltpu.VMEM((length + EDGE, width), bf),
        in_proj=pltpu.VMEM(in_proj.shape, bf),
        branch_proj=pltpu.VMEM(branch_proj.shape, bf),
        inner=pltpu.VMEM((length + EDGE, channels), bf),
        out_proj=pltpu.VMEM(out_proj.shape, bf),
        middle=pltpu.VMEM((unit, width), bf),
        chosen=pltpu.VMEM((unit, width), bf),
        away=pltpu.VMEM((unit, width // 2), bf),
        gate=pltpu.VMEM((4 * depth, hidden_width), bf),
        up=pltpu.VMEM((4 * depth, hidden_width), bf),
        down=pltpu.VMEM(down_proj.shape, bf),
        hidden_in=pltpu.VMEM((2, length, width // 2), bf),
        given=pltpu.VMEM((pieces, length, 2 * PIECE), bf),
        lent=pltpu.VMEM((pieces, length, 2 * PIECE), f32),
        kept=pltpu.VMEM((pieces, length, 2 * PIECE), f32),
        relay=pltpu.VMEM((2, pieces, length // 2, 2 * PIECE), bf),
        taken=pltpu.VMEM((2, pieces, length // 2, 2 * PIECE), bf),
        hidden=pltpu.VMEM((length, hidden_width), bf),
        total=pltpu.VMEM((length, width), f32),
        part=pltpu.VMEM((length, width), bf),
        part2=pltpu.VMEM((length, width), bf),
        gated=pltpu.VMEM((length, channels), bf),
        decays=pltpu.VMEM((length, channels), f32),
        states=pltpu.VMEM((length, channels), f32),
        ends=pltpu.VMEM((8, channels), f32),
        arrived=pltpu.VMEM((count - 1, 8, channels), f32),
        tail_s=dma,
        tail_r=dma,
        end_s=dma((count - 1,)),
        end_r=dma((count - 1,)),
        load=dma((8,)),
        gather_s=dma((2, 2 * CHUNKS)),
        gather_r=dma((2, 2 * CHUNKS)),
        forward_s=dma((2, pieces)),
        forward_r=dma((2, pieces)),
        far_s=dma((1,)),
        far_r=dma((1,)),
        relay_s=dma((2, pieces)),
        relay_r=dma((2, pieces)),
        taken_s=dma((2, pieces)),
        taken_r=dma((2, pieces)),
    )
    return pl.pallas_call(
        functools.partial(layer_kernel, count, conv_weight.shape[0]),
        out_shape=jax.ShapeDtypeStruct((length, width), bf),
        in_specs=[outer] * 16,
        out_specs=pl.BlockSpec(memory_space=pltpu.VMEM),
        scratch_shapes=(
            scratch,
            scatter_scratch(length, width),
            scatter_scratch(length, width),
            gather_scratch(),
            gather_scratch(),
        ),
        compiler_params=pltpu.CompilerParams(
            collective_id=0, has_side_effects=True, vmem_limit_bytes=GRANT
        ),
    )(
        *(
            pltpu.with_memory_space_constraint(array, pltpu.HBM)
            for array in (
                *small,
                residual,
                in_proj,
                branch_proj,
                out_proj,
                gate_proj,
                up_proj,
                down_proj,
            )
        )
    )


def solution(mesh):
    in_specs = (
        P("seq", None),
        P(),
        P(None, "tp"),
        P(None, "tp"),
        P(None, "tp"),
        P("tp"),
        P("tp", None, None),
        P("tp"),
        P("tp", None, None),
        P("tp"),
        P("tp"),
        P("tp", None),
        P(),
        P("seq", "tp"),
        P("seq", "tp"),
        P("tp", None),
    )
    out_specs = P("seq", None)
    return jax.shard_map(
        on_device, mesh=mesh, in_specs=in_specs, out_specs=out_specs, check_vma=False
    )
```

```python
import functools
from types import SimpleNamespace

import jax
import jax.numpy as jnp
from jax import lax
from jax.experimental import pallas as pl
from jax.experimental.pallas import tpu as pltpu
from jax.sharding import PartitionSpec as P

epsilon = 1e-06
LOGICAL = pl.DeviceIdType.MESH
LANES = 128
EDGE = 8
GRANT = 50 * 2**20


def one_minus_exp(x):
    series = 1.0 + x * (1.0 / 9.0)
    for k in range(8, 1, -1):
        series = 1.0 + x * (1.0 / k) * series
    return jnp.where(x > -0.5, -x * series, 1.0 - jnp.exp(x))


def softplus(v):
    small = jnp.exp(-jnp.abs(v))
    whole = 1.0 + small
    grown = jnp.where(whole == 1.0, small, jnp.log(whole) * small / jnp.where(whole == 1.0, 1.0, whole - 1.0))
    return jnp.maximum(v, 0.0) + grown


def local_states(
    taps,
    me,
    inner_ref,
    conv_weight_ref,
    conv_bias_ref,
    input_gate_ref,
    input_bias_ref,
    decay_gate_ref,
    decay_bias_ref,
    decay_param_ref,
    decays_ref,
    states_ref,
    ends_ref,
):
    length, channels = inner_ref.shape[0] - EDGE, inner_ref.shape[1]
    heads, head = input_gate_ref.shape[0], input_gate_ref.shape[1]
    follows = jnp.where(me > 0, 1.0, 0.0)

    for h in range(heads):
        columns = pl.ds(h * head, head)
        row = lax.broadcasted_iota(jnp.int32, (length, head), 0)
        current = inner_ref[:length, columns].astype(jnp.float32)
        tail = inner_ref[length:, columns].astype(jnp.float32) * follows
        before = jnp.concatenate([tail, jnp.zeros((length - EDGE, head), jnp.float32)], axis=0)
        total = conv_bias_ref[:, columns] + conv_weight_ref[0:1, columns] * current
        for tap in range(1, taps):
            shifted = jnp.where(
                row < tap,
                pltpu.roll(before, length + tap - EDGE, 0),
                pltpu.roll(current, tap, 0),
            )
            total = total + conv_weight_ref[tap : tap + 1, columns] * shifted
        smoothed = total.astype(jnp.bfloat16)
        input_rate = jax.nn.sigmoid(
            jnp.dot(smoothed, input_gate_ref[h], preferred_element_type=jnp.float32)
            + input_bias_ref[:, columns]
        )
        decay_rate = jax.nn.sigmoid(
            jnp.dot(smoothed, decay_gate_ref[h], preferred_element_type=jnp.float32)
            + decay_bias_ref[:, columns]
        )
        log_decay = decay_rate * (-8.0 * softplus(decay_param_ref[:, columns]))
        scale_in = jnp.sqrt(one_minus_exp(2.0 * log_decay))
        scale_in = jnp.where(jnp.logical_and(row == 0, me == 0), 1.0, scale_in)
        decays_ref[:, columns] = jnp.exp(log_decay)
        states_ref[:, columns] = smoothed.astype(jnp.float32) * input_rate * scale_in

    for c in range(channels // LANES):
        columns = pl.ds(c * LANES, LANES)
        row = lax.broadcasted_iota(jnp.int32, (length, LANES), 0)
        decay, state = decays_ref[:, columns], states_ref[:, columns]
        step = 1
        while step < length:
            reached = row >= step
            state = state + decay * jnp.where(reached, pltpu.roll(state, step, 0), 0.0)
            decay = decay * jnp.where(reached, pltpu.roll(decay, step, 0), 1.0)
            step *= 2
        decays_ref[:, columns] = decay
        states_ref[:, columns] = state
        ends_ref[0:1, columns] = decay[length - 1 :, :]
        ends_ref[1:2, columns] = state[length - 1 :, :]


def remote(source, target, send, recv, tp, seq):
    return pltpu.make_async_remote_copy(
        src_ref=source,
        dst_ref=target,
        send_sem=send,
        recv_sem=recv,
        device_id={"tp": tp, "seq": seq},
        device_id_type=LOGICAL,
    )


def aligned(index, unit):
    return pl.multiple_of(index * unit, unit)


class Links:
    def __init__(self):
        self.t, self.s = lax.axis_index("tp"), lax.axis_index("seq")
        self.core = lax.rem(self.t, 2)
        self.z = lax.rem(lax.div(self.t, 2), 4)
        self.xl = lax.div(self.t, 8)
        self.xh = lax.rem(self.s, 2)
        self.y = lax.div(self.s, 2)
        t, s, y, z, core = self.t, self.s, self.y, self.z, self.core
        x = 2 * self.xh + self.xl

        def along_z(step):
            return (8 * self.xl + 2 * lax.rem(z + step, 4) + core, s)

        def along_y(step):
            return (t, 2 * lax.rem(y + step, 4) + self.xh)

        def along_x(step):
            other = lax.rem(x + step, 4)
            return (8 * lax.rem(other, 2) + 2 * z + core, 2 * y + lax.div(other, 2))

        self.pair = (t + 1 - 2 * core, s)
        self.z_up, self.z_down = along_z(1), along_z(3)
        self.y_up, self.y_down = along_y(1), along_y(3)
        self.x_up, self.x_down = along_x(1), along_x(3)
        self.near = (8 * (1 - self.xl) + 2 * z + core, s)
        self.far = (t, 2 * y + 1 - self.xh)
        self.outside = (8 * (1 - self.xl) + 2 * z + core, lax.select(self.xl == 0, self.x_down[1], self.x_up[1]))
        self.all_sent = []

    def start(self, source, target, send, recv, device):
        remote(source, target, send, recv, *device).start()

    def arrived(self, target, recv):
        remote(target, target, recv, recv, *self.pair).wait_recv()

    def sent_in_all(self, like, send):
        self.all_sent.append(remote(like, like, send, send, *self.pair))

    def drain(self):
        for copies in self.all_sent:
            copies.wait_send()


GROUPS = 2


def scatter_scratch(length, width):
    bf = jnp.bfloat16
    rows, unit = length // 8, length // 16
    quarter = width // (2 * GROUPS)
    dma = pltpu.SemaphoreType.DMA
    return dict(
        pair=pltpu.VMEM((4, rows, width), bf),
        out_far=pltpu.VMEM((rows, width), bf),
        out_up=pltpu.VMEM((rows, width), bf),
        out_down=pltpu.VMEM((rows, width), bf),
        far_up=pltpu.VMEM((GROUPS, rows, quarter), bf),
        far_down=pltpu.VMEM((GROUPS, rows, quarter), bf),
        from_down=pltpu.VMEM((2 * GROUPS, rows, quarter), bf),
        from_up=pltpu.VMEM((2 * GROUPS, rows, quarter), bf),
        out_near=pltpu.VMEM((unit, width), bf),
        from_near=pltpu.VMEM((GROUPS, unit, 2 * quarter), bf),
        own=pltpu.VMEM((unit, width), jnp.float32),
        pair_s=dma,
        pair_r=dma((4, GROUPS)),
        far_up_r=dma((GROUPS,)),
        far_down_r=dma((GROUPS,)),
        up_s=dma,
        up_r=dma((2 * GROUPS,)),
        down_s=dma,
        down_r=dma((2 * GROUPS,)),
        near_s=dma,
        near_r=dma((GROUPS,)),
    )


def owned_row(links, core, z, xl, unit):
    return aligned(core * 8 + z * 2 + xl, unit)


def pair_up(links, part, b, g):
    rows = b.pair.shape[1]
    width = part.shape[1] // GROUPS
    columns = pl.ds(g * width, width)
    for k, step in enumerate((2, 1, 3, 0)):
        block = (1 - links.core) * 4 + lax.rem(links.z + step, 4)
        links.start(
            part.at[pl.ds(aligned(block, rows), rows), columns],
            b.pair.at[k, :, columns],
            b.pair_s,
            b.pair_r.at[k, g],
            links.pair,
        )


def reduce_scatter(links, part, b, finish):
    rows, width = b.pair.shape[1:]
    unit, quarter = rows // 2, width // (2 * GROUPS)
    order = (2, 1, 3, 0)
    starts = [aligned(links.core * 4 + lax.rem(links.z + step, 4), rows) for step in order]

    def summed(k, q):
        columns = pl.ds(q * quarter, quarter)
        return part[pl.ds(starts[k], rows), columns].astype(jnp.float32) + b.pair[
            k, :, columns
        ].astype(jnp.float32)

    def paired(k, g):
        columns = pl.ds(g * 2 * quarter, 2 * quarter)
        links.arrived(b.pair.at[k, :, columns], b.pair_r.at[k, g])

    def send_far(g):
        paired(0, g)
        for q, landing, send, recv, device in (
            (2 * g, b.far_up, b.up_s, b.far_up_r, links.z_up),
            (2 * g + 1, b.far_down, b.down_s, b.far_down_r, links.z_down),
        ):
            columns = pl.ds(q * quarter, quarter)
            b.out_far[:, columns] = summed(0, q).astype(jnp.bfloat16)
            links.start(b.out_far.at[:, columns], landing.at[g], send, recv.at[g], device)

    def send_up(q, value):
        columns = pl.ds(q * quarter, quarter)
        b.out_up[:, columns] = value.astype(jnp.bfloat16)
        links.start(
            b.out_up.at[:, columns], b.from_down.at[q], b.up_s, b.up_r.at[q], links.z_up
        )

    def send_down(q, value):
        columns = pl.ds(q * quarter, quarter)
        b.out_down[:, columns] = value.astype(jnp.bfloat16)
        links.start(
            b.out_down.at[:, columns], b.from_up.at[q], b.down_s, b.down_r.at[q], links.z_down
        )

    def send_first(g):
        paired(1, g)
        send_up(2 * g + 1, summed(1, 2 * g + 1))
        paired(2, g)
        send_down(2 * g, summed(2, 2 * g))

    def send_second(g):
        links.arrived(b.far_up.at[g], b.far_up_r.at[g])
        send_up(2 * g, summed(1, 2 * g) + b.far_up[g].astype(jnp.float32))
        links.arrived(b.far_down.at[g], b.far_down_r.at[g])
        send_down(2 * g + 1, summed(2, 2 * g + 1) + b.far_down[g].astype(jnp.float32))

    def collect(g):
        paired(3, g)
        for q in (2 * g, 2 * g + 1):
            links.arrived(b.from_down.at[q], b.up_r.at[q])
            links.arrived(b.from_up.at[q], b.down_r.at[q])
            columns = pl.ds(q * quarter, quarter)
            total = (
                summed(3, q)
                + b.from_down[q].astype(jnp.float32)
                + b.from_up[q].astype(jnp.float32)
            )
            low, high = total[:unit], total[unit:]
            first = links.xl == 0
            b.own[:, columns] = jnp.where(first, low, high)
            b.out_near[:, columns] = jnp.where(first, high, low).astype(jnp.bfloat16)
        columns = pl.ds(g * 2 * quarter, 2 * quarter)
        links.start(
            b.out_near.at[:, columns],
            b.from_near.at[g],
            b.near_s,
            b.near_r.at[g],
            links.near,
        )

    for g in range(GROUPS):
        send_far(g)
        if g == 0:
            send_first(0)
    for g in range(GROUPS):
        send_second(g)
        if g + 1 < GROUPS:
            send_first(g + 1)
    for g in range(GROUPS):
        collect(g)
    for g in range(GROUPS):
        links.arrived(b.from_near.at[g], b.near_r.at[g])
        columns = pl.ds(g * 2 * quarter, 2 * quarter)
        finish(columns, b.own[:, columns] + b.from_near[g].astype(jnp.float32))

    links.sent_in_all(part.at[pl.ds(0, 4 * rows), :], b.pair_s)
    links.sent_in_all(part.at[pl.ds(0, 3 * unit), :], b.up_s)
    links.sent_in_all(part.at[pl.ds(0, 3 * unit), :], b.down_s)
    links.sent_in_all(part.at[pl.ds(0, unit), :], b.near_s)


def gather_scratch(pairs):
    dma = pltpu.SemaphoreType.DMA
    return dict(
        near_s=dma,
        near_r=dma((2,)),
        up_s=dma,
        up_r=dma((2, 2)),
        down_s=dma,
        down_r=dma((2, 2)),
        far_up_r=dma((2, 2)),
        far_down_r=dma((2, 2)),
        pair_s=dma,
        pair_r=dma((pairs,)),
    )


class Gather:
    def __init__(self, links, slot, unit, b, pair_of):
        self.links, self.slot, self.unit, self.b, self.pair_of = links, slot, unit, b, pair_of

    def row(self, step, i):
        links = self.links
        across = links.xl if i == 0 else 1 - links.xl
        return owned_row(links, links.core, lax.rem(links.z + step, 4), across, self.unit)

    def pass_on(self, h, r, half=None):
        piece = self.slot(h, r, half)
        self.links.start(piece, piece, self.b.pair_s, self.b.pair_r.at[self.pair_of[h]], self.links.pair)

    def near(self, h):
        piece = self.slot(h, self.row(0, 0), None)
        self.links.start(piece, piece, self.b.near_s, self.b.near_r.at[h], self.links.near)

    def send(self, h, i):
        links, b = self.links, self.b
        piece = self.slot(h, self.row(0, i), None)
        links.start(piece, piece, b.up_s, b.up_r.at[h, i], links.z_up)
        links.start(piece, piece, b.down_s, b.down_r.at[h, i], links.z_down)
        self.pass_on(h, self.row(0, i))

    def from_near(self, h):
        self.links.arrived(self.slot(h, self.row(0, 1), None), self.b.near_r.at[h])
        self.send(h, 1)

    def relay(self, h, i):
        links, b = self.links, self.b
        for step, side, recv, send, far, device in (
            (3, 0, b.up_r, b.up_s, b.far_up_r, links.z_up),
            (1, 1, b.down_r, b.down_s, b.far_down_r, links.z_down),
        ):
            r = self.row(step, i)
            links.arrived(self.slot(h, r, None), recv.at[h, i])
            piece = self.slot(h, r, side)
            links.start(piece, piece, send, far.at[h, i], device)
            self.pass_on(h, r)

    def relayed(self, h, i):
        r = self.row(2, i)
        for side, recv in ((0, self.b.far_up_r), (1, self.b.far_down_r)):
            self.links.arrived(self.slot(h, r, side), recv.at[h, i])
            self.pass_on(h, r, side)


PIECE = 128


CHUNKS = 4


def layer_kernel(
    count,
    taps,
    *refs,
):
    outside, (out_ref, w, first, second, spread, final) = refs[:9], refs[16:]
    residual_ref, in_proj_ref, branch_proj_ref, out_proj_ref, gate_proj_ref, up_proj_ref, down_proj_ref = refs[9:16]
    w, first, second, spread, final = (SimpleNamespace(**s) for s in (w, first, second, spread, final))
    links = Links()
    length, width = residual_ref.shape
    depth, hidden_width = gate_proj_ref.shape
    unit = length // 16
    half = width // 2
    peers = [(links.t, lax.rem(links.s + k, count)) for k in range(1, count)]
    everyone = peers + [links.pair, links.z_up, links.z_down, links.near, links.outside]
    barrier = pltpu.get_barrier_semaphore()
    for tp, seq in everyone:
        pl.semaphore_signal(barrier, inc=1, device_id={"tp": tp, "seq": seq}, device_id_type=LOGICAL)
    own = owned_row(links, links.core, links.z, links.xl, unit)

    behind, here, ahead, opposite = (p * depth for p in range(4))
    loads = [
        pltpu.make_async_copy(residual_ref, w.normed.at[pl.ds(0, length), :], w.load.at[0]),
        pltpu.make_async_copy(in_proj_ref, w.in_proj, w.load.at[1]),
        pltpu.make_async_copy(branch_proj_ref, w.branch_proj, w.load.at[2]),
        pltpu.make_async_copy(out_proj_ref, w.out_proj, w.load.at[3]),
        pltpu.make_async_copy(residual_ref.at[pl.ds(own, unit), :], w.middle, w.load.at[4]),
        pltpu.make_async_copy(gate_proj_ref, w.gate.at[pl.ds(here, depth), :], w.load.at[5]),
        pltpu.make_async_copy(up_proj_ref, w.up.at[pl.ds(here, depth), :], w.load.at[6]),
        pltpu.make_async_copy(down_proj_ref, w.down, w.load.at[7]),
    ]
    small_loads = [
        pltpu.make_async_copy(source, target, w.small_load.at[k])
        for k, (source, target) in enumerate(zip(outside, w.small))
    ]
    for load in loads[:2] + small_loads + loads[2:3]:
        load.start()
    (
        mix_gain_ref,
        conv_weight_ref,
        conv_bias_ref,
        input_gate_ref,
        input_bias_ref,
        decay_gate_ref,
        decay_bias_ref,
        decay_param_ref,
        gain_ref,
    ) = w.small
    pl.semaphore_wait(barrier, len(everyone))

    edge = pl.ds(length, EDGE)
    links.start(
        residual_ref.at[pl.ds(length - EDGE, EDGE), :], w.normed.at[edge, :], w.tail_s, w.tail_r, peers[0]
    )
    share = depth // CHUNKS

    def gather(n):
        rows = pl.ds(n % CHUNKS * share, share)
        sides = ((gate_proj_ref, w.gate), (up_proj_ref, w.up))
        for d, device in enumerate((links.y_up, links.y_down)):
            source, target = sides[(n // CHUNKS + d) % 2]
            there = pl.ds((ahead if d else behind) + n % CHUNKS * share, share)
            links.start(
                source.at[rows, :], target.at[there, :], w.gather_s, w.gather_r.at[d, n // CHUNKS], device
            )

    def gathered(n):
        for d in range(2):
            target = (w.gate, w.up)[(n + d) % 2]
            links.arrived(target.at[pl.ds(ahead if d else behind, depth), :], w.gather_r.at[d, n])

    pieces = hidden_width // PIECE
    onward = ((links.y_up, w.gate, behind), (links.y_down, w.up, ahead))

    def forward(j):
        columns = pl.ds(j * PIECE, PIECE)
        for d, (device, target, start) in enumerate(onward):
            links.start(
                target.at[pl.ds(start, depth), columns],
                target.at[pl.ds(opposite, depth), columns],
                w.forward_s,
                w.forward_r.at[d, j],
                device,
            )

    def forwarded(j):
        columns = pl.ds(j * PIECE, PIECE)
        for d, (device, target, start) in enumerate(onward):
            links.arrived(target.at[pl.ds(opposite, depth), columns], w.forward_r.at[d, j])

    gather(0)
    for load in loads[3:]:
        load.start()

    def norm(start, rows):
        place = pl.ds(start, rows)
        wide = w.normed[place, :].astype(jnp.float32)
        factor = lax.rsqrt(jnp.mean(wide * wide, axis=-1, keepdims=True) + epsilon)
        w.normed[place, :] = (wide * factor * mix_gain_ref[...]).astype(jnp.bfloat16)

    def norm_step(i, carry):
        norm(aligned(i, unit), unit)
        return carry

    for load in small_loads:
        load.wait()
    loads[0].wait()
    lax.fori_loop(0, 16, norm_step, 0)
    links.arrived(w.normed.at[edge, :], w.tail_r)
    norm(length, EDGE)
    loads[1].wait()
    w.inner[...] = jnp.dot(w.normed[...], w.in_proj[...], preferred_element_type=jnp.float32).astype(
        jnp.bfloat16
    )
    local_states(
        taps,
        links.s,
        w.inner,
        conv_weight_ref,
        conv_bias_ref,
        input_gate_ref,
        input_bias_ref,
        decay_gate_ref,
        decay_bias_ref,
        decay_param_ref,
        w.decays,
        w.states,
        w.ends,
    )
    for k in range(count - 1):
        links.start(w.ends, w.arrived.at[k], w.end_s, w.end_r, peers[k])
    for n in range(1, 2 * CHUNKS):
        gather(n)
    loads[2].wait()
    branch = jax.nn.gelu(
        jnp.dot(w.normed[:length, :], w.branch_proj[...], preferred_element_type=jnp.float32), approximate=True
    )
    carried = jnp.zeros((1, w.ends.shape[1]), jnp.float32)
    links.arrived(w.arrived, w.end_r)
    for k in range(count - 2, -1, -1):
        new = w.arrived[k, 0:1, :] * carried + w.arrived[k, 1:2, :]
        carried = jnp.where(links.s >= k + 1, new, carried)
    w.gated[...] = ((w.states[...] + w.decays[...] * carried) * branch).astype(jnp.bfloat16)

    def product(left_ref, right_ref, part_ref, scratch, total_ref=None):
        tile = 512
        for g in range(GROUPS):

            def step(i, carry):
                columns = pl.ds(aligned(i, tile), tile)
                value = jnp.dot(left_ref[...], right_ref[:, columns], preferred_element_type=jnp.float32)
                if total_ref is not None:
                    value = value + total_ref[:, columns]
                part_ref[:, columns] = value.astype(jnp.bfloat16)
                return carry

            steps = width // (GROUPS * tile)
            lax.fori_loop(g * steps, (g + 1) * steps, step, 0)
            pair_up(links, part_ref, scratch, g)

    loads[3].wait()
    product(w.gated, w.out_proj, w.part, first)
    loads[4].wait()

    def to_middle(columns, total):
        w.middle[:, columns] = (total + w.middle[:, columns].astype(jnp.float32)).astype(jnp.bfloat16)

    reduce_scatter(links, w.part, first, to_middle)

    wide = w.middle[...].astype(jnp.float32)
    factor = lax.rsqrt(jnp.mean(wide * wide, axis=-1, keepdims=True) + epsilon)
    w.chosen[...] = (wide * factor * gain_ref[...]).astype(jnp.bfloat16)
    hidden_in = w.hidden_in

    def features(p, which):
        return pl.ds(aligned(2 * lax.rem(links.y + 3 + p, 4) + which, depth), depth)

    def slot(h, r, side):
        group = links.xh if h == 0 else 1 - links.xh
        columns = pl.ds(0, half) if side is None else pl.ds(side * (half // 2), half // 2)
        return hidden_in.at[group, pl.ds(r, unit), columns]

    tokens = Gather(links, slot, unit, spread, (0, 1))
    for p in range(4):
        w.away[:, p * depth : (p + 1) * depth] = w.chosen[:, features(p, 1 - links.xh)]
    landing = hidden_in.at[links.xh, pl.ds(own, unit), :]
    links.start(w.away, landing, w.far_s, w.far_r.at[0], links.far)
    links.start(w.away, landing, w.far_s, w.far_r.at[1], links.outside)
    for p in range(4):
        hidden_in[links.xh, pl.ds(own, unit), p * depth : (p + 1) * depth] = w.chosen[:, features(p, links.xh)]
    tokens.near(0)
    tokens.send(0, 0)
    gathered(0)
    for j in range(pieces):
        forward(j)
    for i in (1, 0):
        links.arrived(slot(1, tokens.row(0, i), None), w.far_r.at[i])
        tokens.send(1, i)
    for i in (1, 0):
        tokens.relay(1, i)
    tokens.relay(0, 0)
    tokens.from_near(0)
    for i in (1, 0):
        tokens.relayed(1, i)
    others = pl.ds(aligned(1 - links.core, length // 2), length // 2)
    links.arrived(hidden_in.at[1 - links.xh, others, :], spread.pair_r.at[1])

    loads[5].wait()
    loads[6].wait()
    gathered(1)

    top = length // 2
    sides = ((links.x_up, 0), (links.x_down, 1))

    def partial(group, j, place):
        return jnp.concatenate(
            [
                jnp.dot(
                    hidden_in[group, :, place],
                    weights[place, j * PIECE : (j + 1) * PIECE],
                    preferred_element_type=jnp.float32,
                )
                for weights in (w.gate, w.up)
            ],
            axis=1,
        )

    nearby, distant = pl.ds(0, opposite), pl.ds(opposite, depth)
    for j in range(pieces):
        w.lent[j] = partial(1 - links.xh, j, nearby)

    def give(j):
        forwarded(j)
        w.given[j] = (w.lent[j] + partial(1 - links.xh, j, distant)).astype(jnp.bfloat16)
        for device, d in sides:
            links.start(
                w.given.at[j, pl.ds(d * top, top), :],
                w.relay.at[d, j],
                w.relay_s,
                w.relay_r.at[d, j],
                device,
            )

    def keep(j):
        w.kept[j] = partial(links.xh, j, pl.ds(0, 4 * depth))

    def pass_on(j):
        for device, d in sides:
            links.arrived(w.relay.at[d, j], w.relay_r.at[d, j])
            links.start(
                w.relay.at[d, j], w.taken.at[d, j], w.taken_s, w.taken_r.at[d, j], device
            )

    def take(j):
        for device, d in sides:
            links.arrived(w.taken.at[d, j], w.taken_r.at[d, j])
            rows = pl.ds(d * top, top)
            both = w.kept[j, rows, :] + w.taken[d, j].astype(jnp.float32)
            w.hidden[rows, j * PIECE : (j + 1) * PIECE] = (
                jax.nn.gelu(both[:, :PIECE], approximate=True) * both[:, PIECE:]
            ).astype(jnp.bfloat16)

    give(0)
    tokens.relay(0, 1)
    for i in range(2):
        tokens.relayed(0, i)
    links.arrived(hidden_in.at[links.xh, others, :], spread.pair_r.at[0])
    give(1)
    for j in range(pieces):
        pass_on(j)
        if j + 2 < pieces:
            give(j + 2)
        keep(j)
        if j > 1:
            take(j - 2)

    loads[7].wait()
    early = (pieces - 2) * PIECE

    def sum_early(i, carry):
        columns = pl.ds(aligned(i, 512), 512)
        w.total[:, columns] = jnp.dot(
            w.hidden[:, :early], w.down[:early, columns], preferred_element_type=jnp.float32
        )
        return carry

    lax.fori_loop(0, width // 512, sum_early, 0)
    take(pieces - 2)
    take(pieces - 1)
    product(w.hidden.at[:, pl.ds(early, 2 * PIECE)], w.down.at[pl.ds(early, 2 * PIECE), :], w.part2, second, w.total)

    def to_out(columns, total):
        out_ref[pl.ds(own, unit), columns] = (
            total + w.middle[:, columns].astype(jnp.float32)
        ).astype(jnp.bfloat16)

    reduce_scatter(links, w.part2, second, to_out)

    def place(h, r, side):
        size = half if side is None else half // 2
        return out_ref.at[pl.ds(r, unit), pl.ds(h * half + (0 if side is None else side * size), size)]

    rows = Gather(links, place, unit, final, (0, 0))
    for h in range(2):
        rows.near(h)
        rows.send(h, 0)
    for h in range(2):
        rows.from_near(h)
    for i in range(2):
        for h in range(2):
            rows.relay(h, i)
    for i in range(2):
        for h in range(2):
            rows.relayed(h, i)
    links.arrived(out_ref.at[others, :], final.pair_r.at[0])

    links.sent_in_all(w.normed.at[edge, :], w.tail_s)
    links.sent_in_all(w.arrived, w.end_s)
    links.sent_in_all(w.gate, w.gather_s)
    links.sent_in_all(w.gate.at[pl.ds(0, 2 * depth), :], w.forward_s)
    links.sent_in_all(w.chosen, w.far_s)
    links.sent_in_all(w.given, w.relay_s)
    links.sent_in_all(w.relay, w.taken_s)
    links.sent_in_all(w.away, spread.near_s)
    links.sent_in_all(w.chosen, final.near_s)
    for b in (spread, final):
        links.sent_in_all(out_ref.at[pl.ds(0, 3 * unit), :], b.up_s)
        links.sent_in_all(out_ref.at[pl.ds(0, 3 * unit), :], b.down_s)
        links.sent_in_all(out_ref.at[others, :], b.pair_s)
    links.drain()


def on_device(
    residual,
    mix_gain,
    in_proj,
    branch_proj,
    conv_weight,
    conv_bias,
    input_gate,
    input_bias,
    decay_gate,
    decay_bias,
    decay_param,
    out_proj,
    mlp_gain,
    gate_proj,
    up_proj,
    down_proj,
):
    count = lax.axis_size("seq")
    length, width = residual.shape
    channels = in_proj.shape[1]
    depth, hidden_width = gate_proj.shape
    unit = length // 16
    bf, f32 = jnp.bfloat16, jnp.float32
    dma = pltpu.SemaphoreType.DMA
    outer = pl.BlockSpec(memory_space=pltpu.HBM)
    pieces = hidden_width // PIECE
    small = (
        mix_gain[None],
        conv_weight,
        conv_bias[None],
        input_gate,
        input_bias[None],
        decay_gate,
        decay_bias[None],
        decay_param[None],
        mlp_gain[None],
    )
    scratch = dict(
        small=tuple(pltpu.VMEM(array.shape, array.dtype) for array in small),
        small_load=dma((len(small),)),
        normed=pltpu.VMEM((length + EDGE, width), bf),
        in_proj=pltpu.VMEM(in_proj.shape, bf),
        branch_proj=pltpu.VMEM(branch_proj.shape, bf),
        inner=pltpu.VMEM((length + EDGE, channels), bf),
        out_proj=pltpu.VMEM(out_proj.shape, bf),
        middle=pltpu.VMEM((unit, width), bf),
        chosen=pltpu.VMEM((unit, width), bf),
        away=pltpu.VMEM((unit, width // 2), bf),
        gate=pltpu.VMEM((4 * depth, hidden_width), bf),
        up=pltpu.VMEM((4 * depth, hidden_width), bf),
        down=pltpu.VMEM(down_proj.shape, bf),
        hidden_in=pltpu.VMEM((2, length, width // 2), bf),
        given=pltpu.VMEM((pieces, length, 2 * PIECE), bf),
        lent=pltpu.VMEM((pieces, length, 2 * PIECE), f32),
        kept=pltpu.VMEM((pieces, length, 2 * PIECE), f32),
        relay=pltpu.VMEM((2, pieces, length // 2, 2 * PIECE), bf),
        taken=pltpu.VMEM((2, pieces, length // 2, 2 * PIECE), bf),
        hidden=pltpu.VMEM((length, hidden_width), bf),
        total=pltpu.VMEM((length, width), f32),
        part=pltpu.VMEM((length, width), bf),
        part2=pltpu.VMEM((length, width), bf),
        gated=pltpu.VMEM((length, channels), bf),
        decays=pltpu.VMEM((length, channels), f32),
        states=pltpu.VMEM((length, channels), f32),
        ends=pltpu.VMEM((8, channels), f32),
        arrived=pltpu.VMEM((count - 1, 8, channels), f32),
        tail_s=dma,
        tail_r=dma,
        end_s=dma,
        end_r=dma,
        load=dma((8,)),
        gather_s=dma,
        gather_r=dma((2, 2)),
        forward_s=dma,
        forward_r=dma((2, pieces)),
        far_s=dma,
        far_r=dma((2,)),
        relay_s=dma,
        relay_r=dma((2, pieces)),
        taken_s=dma,
        taken_r=dma((2, pieces)),
    )
    return pl.pallas_call(
        functools.partial(layer_kernel, count, conv_weight.shape[0]),
        out_shape=jax.ShapeDtypeStruct((length, width), bf),
        in_specs=[outer] * 16,
        out_specs=pl.BlockSpec(memory_space=pltpu.VMEM),
        scratch_shapes=(
            scratch,
            scatter_scratch(length, width),
            scatter_scratch(length, width),
            gather_scratch(2),
            gather_scratch(1),
        ),
        compiler_params=pltpu.CompilerParams(
            collective_id=0, has_side_effects=True, vmem_limit_bytes=GRANT
        ),
    )(
        *(
            pltpu.with_memory_space_constraint(array, pltpu.HBM)
            for array in (
                *small,
                residual,
                in_proj,
                branch_proj,
                out_proj,
                gate_proj,
                up_proj,
                down_proj,
            )
        )
    )


def solution(mesh):
    in_specs = (
        P("seq", None),
        P(),
        P(None, "tp"),
        P(None, "tp"),
        P(None, "tp"),
        P("tp"),
        P("tp", None, None),
        P("tp"),
        P("tp", None, None),
        P("tp"),
        P("tp"),
        P("tp", None),
        P(),
        P("seq", "tp"),
        P("seq", "tp"),
        P("tp", None),
    )
    out_specs = P("seq", None)
    return jax.shard_map(
        on_device, mesh=mesh, in_specs=in_specs, out_specs=out_specs, check_vma=False
    )
```

```python
import functools
from types import SimpleNamespace

import jax
import jax.numpy as jnp
from jax import lax
from jax.experimental import pallas as pl
from jax.experimental.pallas import tpu as pltpu
from jax.sharding import PartitionSpec as P

epsilon = 1e-06
LOGICAL = pl.DeviceIdType.MESH
LANES = 128
EDGE = 8
GRANT = 50 * 2**20


def one_minus_exp(x):
    series = 1.0 + x * (1.0 / 9.0)
    for k in range(8, 1, -1):
        series = 1.0 + x * (1.0 / k) * series
    return jnp.where(x > -0.5, -x * series, 1.0 - jnp.exp(x))


def softplus(v):
    small = jnp.exp(-jnp.abs(v))
    whole = 1.0 + small
    grown = jnp.where(whole == 1.0, small, jnp.log(whole) * small / jnp.where(whole == 1.0, 1.0, whole - 1.0))
    return jnp.maximum(v, 0.0) + grown


def local_states(
    taps,
    me,
    inner_ref,
    conv_weight_ref,
    conv_bias_ref,
    input_gate_ref,
    input_bias_ref,
    decay_gate_ref,
    decay_bias_ref,
    decay_param_ref,
    decays_ref,
    states_ref,
    ends_ref,
):
    length, channels = inner_ref.shape[0] - EDGE, inner_ref.shape[1]
    heads, head = input_gate_ref.shape[0], input_gate_ref.shape[1]
    follows = jnp.where(me > 0, 1.0, 0.0)

    for h in range(heads):
        columns = pl.ds(h * head, head)
        row = lax.broadcasted_iota(jnp.int32, (length, head), 0)
        current = inner_ref[:length, columns].astype(jnp.float32)
        tail = inner_ref[length:, columns].astype(jnp.float32) * follows
        before = jnp.concatenate([tail, jnp.zeros((length - EDGE, head), jnp.float32)], axis=0)
        total = conv_bias_ref[:, columns] + conv_weight_ref[0:1, columns] * current
        for tap in range(1, taps):
            shifted = jnp.where(
                row < tap,
                pltpu.roll(before, length + tap - EDGE, 0),
                pltpu.roll(current, tap, 0),
            )
            total = total + conv_weight_ref[tap : tap + 1, columns] * shifted
        smoothed = total.astype(jnp.bfloat16)
        input_rate = jax.nn.sigmoid(
            jnp.dot(smoothed, input_gate_ref[h], preferred_element_type=jnp.float32)
            + input_bias_ref[:, columns]
        )
        decay_rate = jax.nn.sigmoid(
            jnp.dot(smoothed, decay_gate_ref[h], preferred_element_type=jnp.float32)
            + decay_bias_ref[:, columns]
        )
        log_decay = decay_rate * (-8.0 * softplus(decay_param_ref[:, columns]))
        scale_in = jnp.sqrt(one_minus_exp(2.0 * log_decay))
        scale_in = jnp.where(jnp.logical_and(row == 0, me == 0), 1.0, scale_in)
        decays_ref[:, columns] = jnp.exp(log_decay)
        states_ref[:, columns] = smoothed.astype(jnp.float32) * input_rate * scale_in

    for c in range(channels // LANES):
        columns = pl.ds(c * LANES, LANES)
        row = lax.broadcasted_iota(jnp.int32, (length, LANES), 0)
        decay, state = decays_ref[:, columns], states_ref[:, columns]
        step = 1
        while step < length:
            reached = row >= step
            state = state + decay * jnp.where(reached, pltpu.roll(state, step, 0), 0.0)
            decay = decay * jnp.where(reached, pltpu.roll(decay, step, 0), 1.0)
            step *= 2
        decays_ref[:, columns] = decay
        states_ref[:, columns] = state
        ends_ref[0:1, columns] = decay[length - 1 :, :]
        ends_ref[1:2, columns] = state[length - 1 :, :]


def remote(source, target, send, recv, tp, seq):
    return pltpu.make_async_remote_copy(
        src_ref=source,
        dst_ref=target,
        send_sem=send,
        recv_sem=recv,
        device_id={"tp": tp, "seq": seq},
        device_id_type=LOGICAL,
    )


def aligned(index, unit):
    return pl.multiple_of(index * unit, unit)


class Links:
    def __init__(self):
        self.t, self.s = lax.axis_index("tp"), lax.axis_index("seq")
        self.core = lax.rem(self.t, 2)
        self.z = lax.rem(lax.div(self.t, 2), 4)
        self.xl = lax.div(self.t, 8)
        self.xh = lax.rem(self.s, 2)
        self.y = lax.div(self.s, 2)
        t, s, y, z, core = self.t, self.s, self.y, self.z, self.core
        x = 2 * self.xh + self.xl

        def along_z(step):
            return (8 * self.xl + 2 * lax.rem(z + step, 4) + core, s)

        def along_y(step):
            return (t, 2 * lax.rem(y + step, 4) + self.xh)

        def along_x(step):
            other = lax.rem(x + step, 4)
            return (8 * lax.rem(other, 2) + 2 * z + core, 2 * y + lax.div(other, 2))

        self.pair = (t + 1 - 2 * core, s)
        self.z_up, self.z_down = along_z(1), along_z(3)
        self.y_up, self.y_down = along_y(1), along_y(3)
        self.x_up, self.x_down = along_x(1), along_x(3)
        self.near = (8 * (1 - self.xl) + 2 * z + core, s)
        self.far = (t, 2 * y + 1 - self.xh)
        self.outside = (8 * (1 - self.xl) + 2 * z + core, lax.select(self.xl == 0, self.x_down[1], self.x_up[1]))
        self.all_sent = []

    def start(self, source, target, send, recv, device):
        remote(source, target, send, recv, *device).start()

    def arrived(self, target, recv):
        remote(target, target, recv, recv, *self.pair).wait_recv()

    def sent_in_all(self, like, send):
        self.all_sent.append(remote(like, like, send, send, *self.pair))

    def drain(self):
        for copies in self.all_sent:
            copies.wait_send()


GROUPS = 2


def scatter_scratch(length, width):
    bf = jnp.bfloat16
    rows, unit = length // 8, length // 16
    quarter = width // (2 * GROUPS)
    dma = pltpu.SemaphoreType.DMA
    return dict(
        pair=pltpu.VMEM((4, rows, width), bf),
        out_far=pltpu.VMEM((rows, width), bf),
        out_up=pltpu.VMEM((rows, width), bf),
        out_down=pltpu.VMEM((rows, width), bf),
        far_up=pltpu.VMEM((GROUPS, rows, quarter), bf),
        far_down=pltpu.VMEM((GROUPS, rows, quarter), bf),
        from_down=pltpu.VMEM((2 * GROUPS, rows, quarter), bf),
        from_up=pltpu.VMEM((2 * GROUPS, rows, quarter), bf),
        out_near=pltpu.VMEM((unit, width), bf),
        from_near=pltpu.VMEM((GROUPS, unit, 2 * quarter), bf),
        own=pltpu.VMEM((unit, width), jnp.float32),
        pair_s=dma,
        pair_r=dma((4, GROUPS)),
        far_up_r=dma((GROUPS,)),
        far_down_r=dma((GROUPS,)),
        up_s=dma,
        up_r=dma((2 * GROUPS,)),
        down_s=dma,
        near_s=dma,
        near_r=dma((GROUPS,)),
    )


def owned_row(links, core, z, xl, unit):
    return aligned(core * 8 + z * 2 + xl, unit)


def pair_up(links, part, b, g):
    rows = b.pair.shape[1]
    width = part.shape[1] // GROUPS
    columns = pl.ds(g * width, width)
    for k, step in enumerate((2, 1, 3, 0)):
        block = (1 - links.core) * 4 + lax.rem(links.z + step, 4)
        links.start(
            part.at[pl.ds(aligned(block, rows), rows), columns],
            b.pair.at[k, :, columns],
            b.pair_s,
            b.pair_r.at[k, g],
            links.pair,
        )


def reduce_scatter(links, part, b, finish):
    rows, width = b.pair.shape[1:]
    unit, quarter = rows // 2, width // (2 * GROUPS)
    order = (2, 1, 3, 0)
    starts = [aligned(links.core * 4 + lax.rem(links.z + step, 4), rows) for step in order]

    def summed(k, q):
        columns = pl.ds(q * quarter, quarter)
        return part[pl.ds(starts[k], rows), columns].astype(jnp.float32) + b.pair[
            k, :, columns
        ].astype(jnp.float32)

    def paired(k, g):
        columns = pl.ds(g * 2 * quarter, 2 * quarter)
        links.arrived(b.pair.at[k, :, columns], b.pair_r.at[k, g])

    def send_far(g):
        paired(0, g)
        for q, landing, send, recv, device in (
            (2 * g, b.far_up, b.up_s, b.far_up_r, links.z_up),
            (2 * g + 1, b.far_down, b.down_s, b.far_down_r, links.z_down),
        ):
            columns = pl.ds(q * quarter, quarter)
            b.out_far[:, columns] = summed(0, q).astype(jnp.bfloat16)
            links.start(b.out_far.at[:, columns], landing.at[g], send, recv.at[g], device)

    def send_up(q, value):
        columns = pl.ds(q * quarter, quarter)
        b.out_up[:, columns] = value.astype(jnp.bfloat16)
        links.start(
            b.out_up.at[:, columns], b.from_down.at[q], b.up_s, b.up_r.at[q], links.z_up
        )

    def send_down(q, value):
        columns = pl.ds(q * quarter, quarter)
        b.out_down[:, columns] = value.astype(jnp.bfloat16)
        links.start(
            b.out_down.at[:, columns], b.from_up.at[q], b.down_s, b.up_r.at[q], links.z_down
        )

    def send_first(g):
        paired(1, g)
        send_up(2 * g + 1, summed(1, 2 * g + 1))
        paired(2, g)
        send_down(2 * g, summed(2, 2 * g))

    def send_second(g):
        links.arrived(b.far_up.at[g], b.far_up_r.at[g])
        send_up(2 * g, summed(1, 2 * g) + b.far_up[g].astype(jnp.float32))
        links.arrived(b.far_down.at[g], b.far_down_r.at[g])
        send_down(2 * g + 1, summed(2, 2 * g + 1) + b.far_down[g].astype(jnp.float32))

    def collect(g):
        paired(3, g)
        for q in (2 * g, 2 * g + 1):
            links.arrived(b.from_down.at[pl.ds(0, 2)], b.up_r.at[q])
            columns = pl.ds(q * quarter, quarter)
            total = (
                summed(3, q)
                + b.from_down[q].astype(jnp.float32)
                + b.from_up[q].astype(jnp.float32)
            )
            low, high = total[:unit], total[unit:]
            first = links.xl == 0
            b.own[:, columns] = jnp.where(first, low, high)
            b.out_near[:, columns] = jnp.where(first, high, low).astype(jnp.bfloat16)
        columns = pl.ds(g * 2 * quarter, 2 * quarter)
        links.start(
            b.out_near.at[:, columns],
            b.from_near.at[g],
            b.near_s,
            b.near_r.at[g],
            links.near,
        )

    for g in range(GROUPS):
        send_far(g)
        if g == 0:
            send_first(0)
    for g in range(GROUPS):
        send_second(g)
        if g + 1 < GROUPS:
            send_first(g + 1)
    for g in range(GROUPS):
        collect(g)
    for g in range(GROUPS):
        links.arrived(b.from_near.at[g], b.near_r.at[g])
        columns = pl.ds(g * 2 * quarter, 2 * quarter)
        finish(columns, b.own[:, columns] + b.from_near[g].astype(jnp.float32))

    links.sent_in_all(part.at[pl.ds(0, 4 * rows), :], b.pair_s)
    links.sent_in_all(part.at[pl.ds(0, 3 * unit), :], b.up_s)
    links.sent_in_all(part.at[pl.ds(0, 3 * unit), :], b.down_s)
    links.sent_in_all(part.at[pl.ds(0, unit), :], b.near_s)


def gather_scratch(pairs):
    dma = pltpu.SemaphoreType.DMA
    return dict(
        near_s=dma,
        near_r=dma((2,)),
        up_s=dma,
        up_r=dma((2, 2)),
        down_s=dma,
        down_r=dma((2, 2)),
        far_up_r=dma((2, 2)),
        far_down_r=dma((2, 2)),
        pair_s=dma,
        pair_r=dma((pairs,)),
    )


class Gather:
    def __init__(self, links, slot, unit, b, pair_of):
        self.links, self.slot, self.unit, self.b, self.pair_of = links, slot, unit, b, pair_of

    def row(self, step, i):
        links = self.links
        across = links.xl if i == 0 else 1 - links.xl
        return owned_row(links, links.core, lax.rem(links.z + step, 4), across, self.unit)

    def pass_on(self, h, r, half=None):
        piece = self.slot(h, r, half)
        self.links.start(piece, piece, self.b.pair_s, self.b.pair_r.at[self.pair_of[h]], self.links.pair)

    def near(self, h):
        piece = self.slot(h, self.row(0, 0), None)
        self.links.start(piece, piece, self.b.near_s, self.b.near_r.at[h], self.links.near)

    def send(self, h, i):
        links, b = self.links, self.b
        piece = self.slot(h, self.row(0, i), None)
        links.start(piece, piece, b.up_s, b.up_r.at[h, i], links.z_up)
        links.start(piece, piece, b.down_s, b.down_r.at[h, i], links.z_down)
        self.pass_on(h, self.row(0, i))

    def from_near(self, h):
        self.links.arrived(self.slot(h, self.row(0, 1), None), self.b.near_r.at[h])
        self.send(h, 1)

    def relay(self, h, i):
        links, b = self.links, self.b
        for step, side, recv, send, far, device in (
            (3, 0, b.up_r, b.up_s, b.far_up_r, links.z_up),
            (1, 1, b.down_r, b.down_s, b.far_down_r, links.z_down),
        ):
            r = self.row(step, i)
            links.arrived(self.slot(h, r, None), recv.at[h, i])
            piece = self.slot(h, r, side)
            links.start(piece, piece, send, far.at[h, i], device)
            self.pass_on(h, r)

    def relayed(self, h, i):
        r = self.row(2, i)
        for side, recv in ((0, self.b.far_up_r), (1, self.b.far_down_r)):
            self.links.arrived(self.slot(h, r, side), recv.at[h, i])
            self.pass_on(h, r, side)


PIECE = 128


CHUNKS = 4


def layer_kernel(
    count,
    taps,
    *refs,
):
    outside, (out_ref, w, first, second, spread, final) = refs[:9], refs[16:]
    residual_ref, in_proj_ref, branch_proj_ref, out_proj_ref, gate_proj_ref, up_proj_ref, down_proj_ref = refs[9:16]
    w, first, second, spread, final = (SimpleNamespace(**s) for s in (w, first, second, spread, final))
    links = Links()
    length, width = residual_ref.shape
    depth, hidden_width = gate_proj_ref.shape
    unit = length // 16
    half = width // 2
    peers = [(links.t, lax.rem(links.s + k, count)) for k in range(1, count)]
    everyone = peers + [links.pair, links.z_up, links.z_down, links.near, links.outside]
    barrier = pltpu.get_barrier_semaphore()
    for tp, seq in everyone:
        pl.semaphore_signal(barrier, inc=1, device_id={"tp": tp, "seq": seq}, device_id_type=LOGICAL)
    own = owned_row(links, links.core, links.z, links.xl, unit)

    behind, here, ahead, opposite = (p * depth for p in range(4))
    loads = [
        pltpu.make_async_copy(residual_ref, w.normed.at[pl.ds(0, length), :], w.load.at[0]),
        pltpu.make_async_copy(in_proj_ref, w.in_proj, w.load.at[1]),
        pltpu.make_async_copy(branch_proj_ref, w.branch_proj, w.load.at[2]),
        pltpu.make_async_copy(out_proj_ref, w.out_proj, w.load.at[3]),
        pltpu.make_async_copy(residual_ref.at[pl.ds(own, unit), :], w.middle, w.load.at[4]),
        pltpu.make_async_copy(gate_proj_ref, w.gate.at[pl.ds(here, depth), :], w.load.at[5]),
        pltpu.make_async_copy(up_proj_ref, w.up.at[pl.ds(here, depth), :], w.load.at[6]),
        pltpu.make_async_copy(down_proj_ref, w.down, w.load.at[7]),
    ]
    small_loads = [
        pltpu.make_async_copy(source, target, w.small_load.at[k])
        for k, (source, target) in enumerate(zip(outside, w.small))
    ]
    for load in loads[:2] + small_loads + loads[2:3]:
        load.start()
    (
        mix_gain_ref,
        conv_weight_ref,
        conv_bias_ref,
        input_gate_ref,
        input_bias_ref,
        decay_gate_ref,
        decay_bias_ref,
        decay_param_ref,
        gain_ref,
    ) = w.small
    pl.semaphore_wait(barrier, len(everyone))

    edge = pl.ds(length, EDGE)
    links.start(
        residual_ref.at[pl.ds(length - EDGE, EDGE), :], w.normed.at[edge, :], w.tail_s, w.tail_r, peers[0]
    )
    share = depth // CHUNKS

    def gather(n):
        rows = pl.ds(n % CHUNKS * share, share)
        sides = ((gate_proj_ref, w.gate), (up_proj_ref, w.up))
        for d, device in enumerate((links.y_up, links.y_down)):
            source, target = sides[(n // CHUNKS + d) % 2]
            there = pl.ds((ahead if d else behind) + n % CHUNKS * share, share)
            links.start(
                source.at[rows, :], target.at[there, :], w.gather_s, w.gather_r.at[d, n // CHUNKS], device
            )

    def gathered(n):
        for d in range(2):
            target = (w.gate, w.up)[(n + d) % 2]
            links.arrived(target.at[pl.ds(ahead if d else behind, depth), :], w.gather_r.at[d, n])

    pieces = hidden_width // PIECE
    onward = ((links.y_up, w.gate, behind), (links.y_down, w.up, ahead))

    def forward(j):
        columns = pl.ds(j * PIECE, PIECE)
        for device, target, start in onward:
            links.start(
                target.at[pl.ds(start, depth), columns],
                target.at[pl.ds(opposite, depth), columns],
                w.forward_s,
                w.forward_r.at[j],
                device,
            )

    def forwarded(j):
        columns = pl.ds(j * PIECE, PIECE)
        links.arrived(w.gate.at[pl.ds(ahead, 2 * depth), columns], w.forward_r.at[j])

    for load in loads[3:]:
        load.start()

    def norm(start, rows):
        place = pl.ds(start, rows)
        wide = w.normed[place, :].astype(jnp.float32)
        factor = lax.rsqrt(jnp.mean(wide * wide, axis=-1, keepdims=True) + epsilon)
        w.normed[place, :] = (wide * factor * mix_gain_ref[...]).astype(jnp.bfloat16)

    def norm_step(i, carry):
        norm(aligned(i, unit), unit)
        return carry

    for load in small_loads:
        load.wait()
    loads[0].wait()
    lax.fori_loop(0, 16, norm_step, 0, unroll=4)
    links.arrived(w.normed.at[edge, :], w.tail_r)
    gather(0)
    norm(length, EDGE)
    loads[1].wait()
    w.inner[...] = jnp.dot(w.normed[...], w.in_proj[...], preferred_element_type=jnp.float32).astype(
        jnp.bfloat16
    )
    local_states(
        taps,
        links.s,
        w.inner,
        conv_weight_ref,
        conv_bias_ref,
        input_gate_ref,
        input_bias_ref,
        decay_gate_ref,
        decay_bias_ref,
        decay_param_ref,
        w.decays,
        w.states,
        w.ends,
    )
    for k in range(count - 1):
        links.start(w.ends, w.arrived.at[k], w.end_s, w.end_r, peers[k])
    for n in range(1, 2 * CHUNKS):
        gather(n)
    loads[2].wait()
    branch = jax.nn.gelu(
        jnp.dot(w.normed[:length, :], w.branch_proj[...], preferred_element_type=jnp.float32), approximate=True
    )
    carried = jnp.zeros((1, w.ends.shape[1]), jnp.float32)
    links.arrived(w.arrived, w.end_r)
    for k in range(count - 2, -1, -1):
        new = w.arrived[k, 0:1, :] * carried + w.arrived[k, 1:2, :]
        carried = jnp.where(links.s >= k + 1, new, carried)
    w.gated[...] = ((w.states[...] + w.decays[...] * carried) * branch).astype(jnp.bfloat16)

    def product(left_ref, right_ref, part_ref, scratch, total_ref=None):
        tile = 512
        for g in range(GROUPS):

            def step(i, carry):
                columns = pl.ds(aligned(i, tile), tile)
                value = jnp.dot(left_ref[...], right_ref[:, columns], preferred_element_type=jnp.float32)
                if total_ref is not None:
                    value = value + total_ref[:, columns]
                part_ref[:, columns] = value.astype(jnp.bfloat16)
                return carry

            steps = width // (GROUPS * tile)
            lax.fori_loop(g * steps, (g + 1) * steps, step, 0, unroll=True)
            pair_up(links, part_ref, scratch, g)

    loads[3].wait()
    product(w.gated, w.out_proj, w.part, first)
    loads[4].wait()

    def to_middle(columns, total):
        w.middle[:, columns] = (total + w.middle[:, columns].astype(jnp.float32)).astype(jnp.bfloat16)

    reduce_scatter(links, w.part, first, to_middle)

    wide = w.middle[...].astype(jnp.float32)
    factor = lax.rsqrt(jnp.mean(wide * wide, axis=-1, keepdims=True) + epsilon)
    w.chosen[...] = (wide * factor * gain_ref[...]).astype(jnp.bfloat16)
    hidden_in = w.hidden_in

    def features(p, which):
        return pl.ds(aligned(2 * lax.rem(links.y + 3 + p, 4) + which, depth), depth)

    def slot(h, r, side):
        group = links.xh if h == 0 else 1 - links.xh
        columns = pl.ds(0, half) if side is None else pl.ds(side * (half // 2), half // 2)
        return hidden_in.at[group, pl.ds(r, unit), columns]

    tokens = Gather(links, slot, unit, spread, (0, 1))
    for p in range(4):
        w.away[:, p * depth : (p + 1) * depth] = w.chosen[:, features(p, 1 - links.xh)]
    landing = hidden_in.at[links.xh, pl.ds(own, unit), :]
    links.start(w.away, landing, w.far_s, w.far_r.at[0], links.far)
    links.start(w.away, landing, w.far_s, w.far_r.at[1], links.outside)
    for p in range(4):
        hidden_in[links.xh, pl.ds(own, unit), p * depth : (p + 1) * depth] = w.chosen[:, features(p, links.xh)]
    tokens.near(0)
    tokens.send(0, 0)
    gathered(0)
    for j in range(pieces):
        forward(j)
    for i in (1, 0):
        links.arrived(slot(1, tokens.row(0, i), None), w.far_r.at[i])
        tokens.send(1, i)
    for i in (1, 0):
        tokens.relay(1, i)
    tokens.relay(0, 0)
    tokens.from_near(0)
    for i in (1, 0):
        tokens.relayed(1, i)
    others = pl.ds(aligned(1 - links.core, length // 2), length // 2)
    links.arrived(hidden_in.at[1 - links.xh, others, :], spread.pair_r.at[1])

    loads[5].wait()
    loads[6].wait()
    gathered(1)

    top = length // 2
    sides = ((links.x_up, 0), (links.x_down, 1))

    def partial(group, j):
        return jnp.concatenate(
            [
                jnp.dot(
                    hidden_in[group],
                    weights[:, j * PIECE : (j + 1) * PIECE],
                    preferred_element_type=jnp.float32,
                )
                for weights in (w.gate, w.up)
            ],
            axis=1,
        )

    def give(j):
        forwarded(j)
        w.given[j] = partial(1 - links.xh, j).astype(jnp.bfloat16)
        for device, d in sides:
            links.start(
                w.given.at[j, pl.ds(d * top, top), :],
                w.relay.at[d, j],
                w.relay_s,
                w.relay_r.at[j],
                device,
            )

    def keep(j):
        w.kept[j] = partial(links.xh, j)

    def pass_on(j):
        links.arrived(w.relay.at[:, j], w.relay_r.at[j])
        for device, d in sides:
            links.start(
                w.relay.at[d, j], w.taken.at[d, j], w.taken_s, w.taken_r.at[j], device
            )

    def take(j):
        links.arrived(w.taken.at[:, j], w.taken_r.at[j])
        for device, d in sides:
            rows = pl.ds(d * top, top)
            both = w.kept[j, rows, :] + w.taken[d, j].astype(jnp.float32)
            w.hidden[rows, j * PIECE : (j + 1) * PIECE] = (
                jax.nn.gelu(both[:, :PIECE], approximate=True) * both[:, PIECE:]
            ).astype(jnp.bfloat16)

    give(0)
    give(1)
    tokens.relay(0, 1)
    for j in range(pieces):
        pass_on(j)
        if j + 2 < pieces:
            give(j + 2)
        if j == 0:
            for i in range(2):
                tokens.relayed(0, i)
            links.arrived(hidden_in.at[links.xh, others, :], spread.pair_r.at[0])
        keep(j)
        if j > 1:
            take(j - 2)

    loads[7].wait()
    early = (pieces - 2) * PIECE

    def sum_early(i, carry):
        columns = pl.ds(aligned(i, 512), 512)
        w.total[:, columns] = jnp.dot(
            w.hidden[:, :early], w.down[:early, columns], preferred_element_type=jnp.float32
        )
        return carry

    lax.fori_loop(0, width // 512, sum_early, 0, unroll=4)
    take(pieces - 2)
    take(pieces - 1)
    product(w.hidden.at[:, pl.ds(early, 2 * PIECE)], w.down.at[pl.ds(early, 2 * PIECE), :], w.part2, second, w.total)

    def to_out(columns, total):
        out_ref[pl.ds(own, unit), columns] = (
            total + w.middle[:, columns].astype(jnp.float32)
        ).astype(jnp.bfloat16)

    reduce_scatter(links, w.part2, second, to_out)

    def place(h, r, side):
        size = half if side is None else half // 2
        return out_ref.at[pl.ds(r, unit), pl.ds(h * half + (0 if side is None else side * size), size)]

    rows = Gather(links, place, unit, final, (0, 0))
    for h in range(2):
        rows.near(h)
        rows.send(h, 0)
    for h in range(2):
        rows.from_near(h)
    for i in range(2):
        for h in range(2):
            rows.relay(h, i)
    for i in range(2):
        for h in range(2):
            rows.relayed(h, i)
    links.arrived(out_ref.at[others, :], final.pair_r.at[0])

    links.sent_in_all(w.normed.at[edge, :], w.tail_s)
    links.sent_in_all(w.arrived, w.end_s)
    links.sent_in_all(w.gate, w.gather_s)
    links.sent_in_all(w.gate.at[pl.ds(0, 2 * depth), :], w.forward_s)
    links.sent_in_all(w.chosen, w.far_s)
    links.sent_in_all(w.given, w.relay_s)
    links.sent_in_all(w.relay, w.taken_s)
    links.sent_in_all(w.away, spread.near_s)
    links.sent_in_all(w.chosen, final.near_s)
    for b in (spread, final):
        links.sent_in_all(out_ref.at[pl.ds(0, 3 * unit), :], b.up_s)
        links.sent_in_all(out_ref.at[pl.ds(0, 3 * unit), :], b.down_s)
        links.sent_in_all(out_ref.at[others, :], b.pair_s)
    links.drain()


def on_device(
    residual,
    mix_gain,
    in_proj,
    branch_proj,
    conv_weight,
    conv_bias,
    input_gate,
    input_bias,
    decay_gate,
    decay_bias,
    decay_param,
    out_proj,
    mlp_gain,
    gate_proj,
    up_proj,
    down_proj,
):
    count = lax.axis_size("seq")
    length, width = residual.shape
    channels = in_proj.shape[1]
    depth, hidden_width = gate_proj.shape
    unit = length // 16
    bf, f32 = jnp.bfloat16, jnp.float32
    dma = pltpu.SemaphoreType.DMA
    outer = pl.BlockSpec(memory_space=pltpu.HBM)
    pieces = hidden_width // PIECE
    small = (
        mix_gain[None],
        conv_weight,
        conv_bias[None],
        input_gate,
        input_bias[None],
        decay_gate,
        decay_bias[None],
        decay_param[None],
        mlp_gain[None],
    )
    scratch = dict(
        small=tuple(pltpu.VMEM(array.shape, array.dtype) for array in small),
        small_load=dma((len(small),)),
        normed=pltpu.VMEM((length + EDGE, width), bf),
        in_proj=pltpu.VMEM(in_proj.shape, bf),
        branch_proj=pltpu.VMEM(branch_proj.shape, bf),
        inner=pltpu.VMEM((length + EDGE, channels), bf),
        out_proj=pltpu.VMEM(out_proj.shape, bf),
        middle=pltpu.VMEM((unit, width), bf),
        chosen=pltpu.VMEM((unit, width), bf),
        away=pltpu.VMEM((unit, width // 2), bf),
        gate=pltpu.VMEM((4 * depth, hidden_width), bf),
        up=pltpu.VMEM((4 * depth, hidden_width), bf),
        down=pltpu.VMEM(down_proj.shape, bf),
        hidden_in=pltpu.VMEM((2, length, width // 2), bf),
        given=pltpu.VMEM((pieces, length, 2 * PIECE), bf),
        kept=pltpu.VMEM((pieces, length, 2 * PIECE), f32),
        relay=pltpu.VMEM((2, pieces, length // 2, 2 * PIECE), bf),
        taken=pltpu.VMEM((2, pieces, length // 2, 2 * PIECE), bf),
        hidden=pltpu.VMEM((length, hidden_width), bf),
        total=pltpu.VMEM((length, width), f32),
        part=pltpu.VMEM((length, width), bf),
        part2=pltpu.VMEM((length, width), bf),
        gated=pltpu.VMEM((length, channels), bf),
        decays=pltpu.VMEM((length, channels), f32),
        states=pltpu.VMEM((length, channels), f32),
        ends=pltpu.VMEM((8, channels), f32),
        arrived=pltpu.VMEM((count - 1, 8, channels), f32),
        tail_s=dma,
        tail_r=dma,
        end_s=dma,
        end_r=dma,
        load=dma((8,)),
        gather_s=dma,
        gather_r=dma((2, 2)),
        forward_s=dma,
        forward_r=dma((pieces,)),
        far_s=dma,
        far_r=dma((2,)),
        relay_s=dma,
        relay_r=dma((pieces,)),
        taken_s=dma,
        taken_r=dma((pieces,)),
    )
    return pl.pallas_call(
        functools.partial(layer_kernel, count, conv_weight.shape[0]),
        out_shape=jax.ShapeDtypeStruct((length, width), bf),
        in_specs=[outer] * 16,
        out_specs=pl.BlockSpec(memory_space=pltpu.VMEM),
        scratch_shapes=(
            scratch,
            scatter_scratch(length, width),
            scatter_scratch(length, width),
            gather_scratch(2),
            gather_scratch(1),
        ),
        compiler_params=pltpu.CompilerParams(
            collective_id=0, has_side_effects=True, vmem_limit_bytes=GRANT
        ),
    )(
        *(
            pltpu.with_memory_space_constraint(array, pltpu.HBM)
            for array in (
                *small,
                residual,
                in_proj,
                branch_proj,
                out_proj,
                gate_proj,
                up_proj,
                down_proj,
            )
        )
    )


def solution(mesh):
    in_specs = (
        P("seq", None),
        P(),
        P(None, "tp"),
        P(None, "tp"),
        P(None, "tp"),
        P("tp"),
        P("tp", None, None),
        P("tp"),
        P("tp", None, None),
        P("tp"),
        P("tp"),
        P("tp", None),
        P(),
        P("seq", "tp"),
        P("seq", "tp"),
        P("tp", None),
    )
    out_specs = P("seq", None)
    return jax.shard_map(
        on_device, mesh=mesh, in_specs=in_specs, out_specs=out_specs, check_vma=False
    )
```

```python
import functools
from types import SimpleNamespace

import jax
import jax.numpy as jnp
from jax import lax
from jax.experimental import pallas as pl
from jax.experimental.pallas import tpu as pltpu
from jax.sharding import PartitionSpec as P

epsilon = 1e-06
LOGICAL = pl.DeviceIdType.MESH
LANES = 128
EDGE = 8
GRANT = 50 * 2**20


def one_minus_exp(x):
    series = 1.0 + x * (1.0 / 9.0)
    for k in range(8, 1, -1):
        series = 1.0 + x * (1.0 / k) * series
    return jnp.where(x > -0.5, -x * series, 1.0 - jnp.exp(x))


def softplus(v):
    small = jnp.exp(-jnp.abs(v))
    whole = 1.0 + small
    grown = jnp.where(whole == 1.0, small, jnp.log(whole) * small / jnp.where(whole == 1.0, 1.0, whole - 1.0))
    return jnp.maximum(v, 0.0) + grown


def local_states(
    taps,
    me,
    inner_ref,
    conv_weight_ref,
    conv_bias_ref,
    input_gate_ref,
    input_bias_ref,
    decay_gate_ref,
    decay_bias_ref,
    decay_param_ref,
    decays_ref,
    states_ref,
    ends_ref,
):
    length, channels = inner_ref.shape[0] - EDGE, inner_ref.shape[1]
    heads, head = input_gate_ref.shape[0], input_gate_ref.shape[1]
    follows = jnp.where(me > 0, 1.0, 0.0)

    for h in range(heads):
        columns = pl.ds(h * head, head)
        row = lax.broadcasted_iota(jnp.int32, (length, head), 0)
        current = inner_ref[:length, columns].astype(jnp.float32)
        tail = inner_ref[length:, columns].astype(jnp.float32) * follows
        before = jnp.concatenate([tail, jnp.zeros((length - EDGE, head), jnp.float32)], axis=0)
        total = conv_bias_ref[:, columns] + conv_weight_ref[0:1, columns] * current
        for tap in range(1, taps):
            shifted = jnp.where(
                row < tap,
                pltpu.roll(before, length + tap - EDGE, 0),
                pltpu.roll(current, tap, 0),
            )
            total = total + conv_weight_ref[tap : tap + 1, columns] * shifted
        smoothed = total.astype(jnp.bfloat16)
        input_rate = jax.nn.sigmoid(
            jnp.dot(smoothed, input_gate_ref[h], preferred_element_type=jnp.float32)
            + input_bias_ref[:, columns]
        )
        decay_rate = jax.nn.sigmoid(
            jnp.dot(smoothed, decay_gate_ref[h], preferred_element_type=jnp.float32)
            + decay_bias_ref[:, columns]
        )
        log_decay = decay_rate * (-8.0 * softplus(decay_param_ref[:, columns]))
        scale_in = jnp.sqrt(one_minus_exp(2.0 * log_decay))
        scale_in = jnp.where(jnp.logical_and(row == 0, me == 0), 1.0, scale_in)
        decays_ref[:, columns] = jnp.exp(log_decay)
        states_ref[:, columns] = smoothed.astype(jnp.float32) * input_rate * scale_in

    for c in range(channels // LANES):
        columns = pl.ds(c * LANES, LANES)
        row = lax.broadcasted_iota(jnp.int32, (length, LANES), 0)
        decay, state = decays_ref[:, columns], states_ref[:, columns]
        step = 1
        while step < length:
            reached = row >= step
            state = state + decay * jnp.where(reached, pltpu.roll(state, step, 0), 0.0)
            decay = decay * jnp.where(reached, pltpu.roll(decay, step, 0), 1.0)
            step *= 2
        decays_ref[:, columns] = decay
        states_ref[:, columns] = state
        ends_ref[0:1, columns] = decay[length - 1 :, :]
        ends_ref[1:2, columns] = state[length - 1 :, :]


def remote(source, target, send, recv, tp, seq):
    return pltpu.make_async_remote_copy(
        src_ref=source,
        dst_ref=target,
        send_sem=send,
        recv_sem=recv,
        device_id={"tp": tp, "seq": seq},
        device_id_type=LOGICAL,
    )


def aligned(index, unit):
    return pl.multiple_of(index * unit, unit)


class Links:
    def __init__(self):
        self.t, self.s = lax.axis_index("tp"), lax.axis_index("seq")
        self.core = lax.rem(self.t, 2)
        self.z = lax.rem(lax.div(self.t, 2), 4)
        self.xl = lax.div(self.t, 8)
        self.xh = lax.rem(self.s, 2)
        self.y = lax.div(self.s, 2)
        t, s, y, z, core = self.t, self.s, self.y, self.z, self.core
        x = 2 * self.xh + self.xl

        def along_z(step):
            return (8 * self.xl + 2 * lax.rem(z + step, 4) + core, s)

        def along_y(step):
            return (t, 2 * lax.rem(y + step, 4) + self.xh)

        def along_x(step):
            other = lax.rem(x + step, 4)
            return (8 * lax.rem(other, 2) + 2 * z + core, 2 * y + lax.div(other, 2))

        self.pair = (t + 1 - 2 * core, s)
        self.z_up, self.z_down = along_z(1), along_z(3)
        self.y_up, self.y_down = along_y(1), along_y(3)
        self.x_up, self.x_down = along_x(1), along_x(3)
        self.near = (8 * (1 - self.xl) + 2 * z + core, s)
        self.far = (t, 2 * y + 1 - self.xh)
        self.outside = (8 * (1 - self.xl) + 2 * z + core, lax.select(self.xl == 0, self.x_down[1], self.x_up[1]))
        self.all_sent = []

    def start(self, source, target, send, recv, device):
        remote(source, target, send, recv, *device).start()

    def arrived(self, target, recv):
        remote(target, target, recv, recv, *self.pair).wait_recv()

    def sent_in_all(self, like, send):
        self.all_sent.append(remote(like, like, send, send, *self.pair))

    def drain(self):
        for copies in self.all_sent:
            copies.wait_send()


GROUPS = 2


def scatter_scratch(length, width):
    bf = jnp.bfloat16
    rows, unit = length // 8, length // 16
    quarter = width // (2 * GROUPS)
    dma = pltpu.SemaphoreType.DMA
    return dict(
        pair=pltpu.VMEM((4, rows, width), bf),
        out_far=pltpu.VMEM((rows, width), bf),
        out_up=pltpu.VMEM((rows, width), bf),
        out_down=pltpu.VMEM((rows, width), bf),
        far_up=pltpu.VMEM((GROUPS, rows, quarter), bf),
        far_down=pltpu.VMEM((GROUPS, rows, quarter), bf),
        from_down=pltpu.VMEM((2 * GROUPS, rows, quarter), bf),
        from_up=pltpu.VMEM((2 * GROUPS, rows, quarter), bf),
        out_near=pltpu.VMEM((unit, width), bf),
        from_near=pltpu.VMEM((GROUPS, unit, 2 * quarter), bf),
        own=pltpu.VMEM((unit, width), jnp.float32),
        pair_s=dma,
        pair_r=dma((4, GROUPS)),
        far_up_r=dma((GROUPS,)),
        far_down_r=dma((GROUPS,)),
        up_s=dma,
        up_r=dma((2 * GROUPS,)),
        down_s=dma,
        near_s=dma,
        near_r=dma((GROUPS,)),
    )


def owned_row(links, core, z, xl, unit):
    return aligned(core * 8 + z * 2 + xl, unit)


def pair_up(links, part, b, g):
    rows = b.pair.shape[1]
    width = part.shape[1] // GROUPS
    columns = pl.ds(g * width, width)
    for k, step in enumerate((2, 1, 3, 0)):
        block = (1 - links.core) * 4 + lax.rem(links.z + step, 4)
        links.start(
            part.at[pl.ds(aligned(block, rows), rows), columns],
            b.pair.at[k, :, columns],
            b.pair_s,
            b.pair_r.at[k, g],
            links.pair,
        )


def reduce_scatter(links, part, b, finish):
    rows, width = b.pair.shape[1:]
    unit, quarter = rows // 2, width // (2 * GROUPS)
    order = (2, 1, 3, 0)
    starts = [aligned(links.core * 4 + lax.rem(links.z + step, 4), rows) for step in order]

    def summed(k, q):
        columns = pl.ds(q * quarter, quarter)
        return part[pl.ds(starts[k], rows), columns].astype(jnp.float32) + b.pair[
            k, :, columns
        ].astype(jnp.float32)

    def paired(k, g):
        columns = pl.ds(g * 2 * quarter, 2 * quarter)
        links.arrived(b.pair.at[k, :, columns], b.pair_r.at[k, g])

    def send_far(g):
        paired(0, g)
        for q, landing, send, recv, device in (
            (2 * g, b.far_up, b.up_s, b.far_up_r, links.z_up),
            (2 * g + 1, b.far_down, b.down_s, b.far_down_r, links.z_down),
        ):
            columns = pl.ds(q * quarter, quarter)
            b.out_far[:, columns] = summed(0, q).astype(jnp.bfloat16)
            links.start(b.out_far.at[:, columns], landing.at[g], send, recv.at[g], device)

    def send_up(q, value):
        columns = pl.ds(q * quarter, quarter)
        b.out_up[:, columns] = value.astype(jnp.bfloat16)
        links.start(
            b.out_up.at[:, columns], b.from_down.at[q], b.up_s, b.up_r.at[q], links.z_up
        )

    def send_down(q, value):
        columns = pl.ds(q * quarter, quarter)
        b.out_down[:, columns] = value.astype(jnp.bfloat16)
        links.start(
            b.out_down.at[:, columns], b.from_up.at[q], b.down_s, b.up_r.at[q], links.z_down
        )

    def send_first(g):
        paired(1, g)
        send_up(2 * g + 1, summed(1, 2 * g + 1))
        paired(2, g)
        send_down(2 * g, summed(2, 2 * g))

    def send_second(g):
        links.arrived(b.far_up.at[g], b.far_up_r.at[g])
        send_up(2 * g, summed(1, 2 * g) + b.far_up[g].astype(jnp.float32))
        links.arrived(b.far_down.at[g], b.far_down_r.at[g])
        send_down(2 * g + 1, summed(2, 2 * g + 1) + b.far_down[g].astype(jnp.float32))

    def collect(g):
        paired(3, g)
        for q in (2 * g, 2 * g + 1):
            links.arrived(b.from_down.at[pl.ds(0, 2)], b.up_r.at[q])
            columns = pl.ds(q * quarter, quarter)
            total = (
                summed(3, q)
                + b.from_down[q].astype(jnp.float32)
                + b.from_up[q].astype(jnp.float32)
            )
            low, high = total[:unit], total[unit:]
            first = links.xl == 0
            b.own[:, columns] = jnp.where(first, low, high)
            b.out_near[:, columns] = jnp.where(first, high, low).astype(jnp.bfloat16)
        columns = pl.ds(g * 2 * quarter, 2 * quarter)
        links.start(
            b.out_near.at[:, columns],
            b.from_near.at[g],
            b.near_s,
            b.near_r.at[g],
            links.near,
        )

    for g in range(GROUPS):
        send_far(g)
        if g == 0:
            send_first(0)
    for g in range(GROUPS):
        send_second(g)
        if g + 1 < GROUPS:
            send_first(g + 1)
    for g in range(GROUPS):
        collect(g)
    for g in range(GROUPS):
        links.arrived(b.from_near.at[g], b.near_r.at[g])
        columns = pl.ds(g * 2 * quarter, 2 * quarter)
        finish(columns, b.own[:, columns] + b.from_near[g].astype(jnp.float32))

    links.sent_in_all(part.at[pl.ds(0, 4 * rows), :], b.pair_s)
    links.sent_in_all(part.at[pl.ds(0, 3 * unit), :], b.up_s)
    links.sent_in_all(part.at[pl.ds(0, 3 * unit), :], b.down_s)
    links.sent_in_all(part.at[pl.ds(0, unit), :], b.near_s)


def gather_scratch(pairs):
    dma = pltpu.SemaphoreType.DMA
    return dict(
        near_s=dma,
        near_r=dma((2,)),
        up_s=dma,
        up_r=dma((2, 2)),
        down_s=dma,
        down_r=dma((2, 2)),
        far_up_r=dma((2, 2)),
        far_down_r=dma((2, 2)),
        pair_s=dma,
        pair_r=dma((pairs,)),
    )


class Gather:
    def __init__(self, links, slot, unit, b, pair_of):
        self.links, self.slot, self.unit, self.b, self.pair_of = links, slot, unit, b, pair_of

    def row(self, step, i):
        links = self.links
        across = links.xl if i == 0 else 1 - links.xl
        return owned_row(links, links.core, lax.rem(links.z + step, 4), across, self.unit)

    def pass_on(self, h, r, half=None):
        piece = self.slot(h, r, half)
        self.links.start(piece, piece, self.b.pair_s, self.b.pair_r.at[self.pair_of[h]], self.links.pair)

    def near(self, h):
        piece = self.slot(h, self.row(0, 0), None)
        self.links.start(piece, piece, self.b.near_s, self.b.near_r.at[h], self.links.near)

    def send(self, h, i):
        links, b = self.links, self.b
        piece = self.slot(h, self.row(0, i), None)
        links.start(piece, piece, b.up_s, b.up_r.at[h, i], links.z_up)
        links.start(piece, piece, b.down_s, b.down_r.at[h, i], links.z_down)
        self.pass_on(h, self.row(0, i))

    def from_near(self, h):
        self.links.arrived(self.slot(h, self.row(0, 1), None), self.b.near_r.at[h])
        self.send(h, 1)

    def relay(self, h, i):
        links, b = self.links, self.b
        for step, side, recv, send, far, device in (
            (3, 0, b.up_r, b.up_s, b.far_up_r, links.z_up),
            (1, 1, b.down_r, b.down_s, b.far_down_r, links.z_down),
        ):
            r = self.row(step, i)
            links.arrived(self.slot(h, r, None), recv.at[h, i])
            piece = self.slot(h, r, side)
            links.start(piece, piece, send, far.at[h, i], device)
            self.pass_on(h, r)

    def relayed(self, h, i):
        r = self.row(2, i)
        for side, recv in ((0, self.b.far_up_r), (1, self.b.far_down_r)):
            self.links.arrived(self.slot(h, r, side), recv.at[h, i])
            self.pass_on(h, r, side)


PIECE = 128


CHUNKS = 8
PARTS = 4


def layer_kernel(
    count,
    taps,
    *refs,
):
    outside, (out_ref, w, first, second, spread, final) = refs[:9], refs[16:]
    residual_ref, in_proj_ref, branch_proj_ref, out_proj_ref, gate_proj_ref, up_proj_ref, down_proj_ref = refs[9:16]
    w, first, second, spread, final = (SimpleNamespace(**s) for s in (w, first, second, spread, final))
    links = Links()
    length, width = residual_ref.shape
    depth, hidden_width = gate_proj_ref.shape
    unit = length // 16
    half = width // 2
    peers = [(links.t, lax.rem(links.s + k, count)) for k in range(1, count)]
    everyone = peers + [links.pair, links.z_up, links.z_down, links.near, links.outside]
    barrier = pltpu.get_barrier_semaphore()
    for tp, seq in everyone:
        pl.semaphore_signal(barrier, inc=1, device_id={"tp": tp, "seq": seq}, device_id_type=LOGICAL)
    own = owned_row(links, links.core, links.z, links.xl, unit)

    behind, here, ahead, opposite = (p * depth for p in range(4))
    loads = [
        pltpu.make_async_copy(residual_ref.at[pl.ds(length - EDGE, EDGE), :], w.edge, w.load.at[0]),
        pltpu.make_async_copy(in_proj_ref, w.in_proj, w.load.at[1]),
        pltpu.make_async_copy(branch_proj_ref, w.branch_proj, w.load.at[2]),
        pltpu.make_async_copy(out_proj_ref, w.out_proj, w.load.at[3]),
        pltpu.make_async_copy(residual_ref.at[pl.ds(own, unit), :], w.middle, w.load.at[4]),
        pltpu.make_async_copy(gate_proj_ref, w.gate.at[pl.ds(here, depth), :], w.load.at[5]),
        pltpu.make_async_copy(up_proj_ref, w.up.at[pl.ds(here, depth), :], w.load.at[6]),
        pltpu.make_async_copy(down_proj_ref, w.down, w.load.at[7]),
    ]
    part_rows = length // PARTS
    row_loads = [
        pltpu.make_async_copy(
            residual_ref.at[pl.ds(k * part_rows, part_rows), :],
            w.normed.at[pl.ds(k * part_rows, part_rows), :],
            w.row_load.at[k],
        )
        for k in range(PARTS)
    ]
    small_loads = [
        pltpu.make_async_copy(source, target, w.small_load.at[k])
        for k, (source, target) in enumerate(zip(outside, w.small))
    ]
    for load in loads[:1] + small_loads[:1] + row_loads + loads[1:2] + small_loads[1:] + loads[2:3]:
        load.start()
    (
        mix_gain_ref,
        conv_weight_ref,
        conv_bias_ref,
        input_gate_ref,
        input_bias_ref,
        decay_gate_ref,
        decay_bias_ref,
        decay_param_ref,
        gain_ref,
    ) = w.small
    pl.semaphore_wait(barrier, len(everyone))

    edge = pl.ds(length, EDGE)
    loads[0].wait()
    links.start(w.edge, w.normed.at[edge, :], w.tail_s, w.tail_r, peers[0])
    share = depth // CHUNKS

    def gather(n):
        rows = pl.ds(n % CHUNKS * share, share)
        sides = ((gate_proj_ref, w.gate), (up_proj_ref, w.up))
        for d, device in enumerate((links.y_up, links.y_down)):
            source, target = sides[(n // CHUNKS + d) % 2]
            there = pl.ds((ahead if d else behind) + n % CHUNKS * share, share)
            links.start(
                source.at[rows, :], target.at[there, :], w.gather_s, w.gather_r.at[d, n // CHUNKS], device
            )

    def gathered(n):
        for d in range(2):
            target = (w.gate, w.up)[(n + d) % 2]
            links.arrived(target.at[pl.ds(ahead if d else behind, depth), :], w.gather_r.at[d, n])

    pieces = hidden_width // PIECE
    onward = ((links.y_up, w.gate, behind), (links.y_down, w.up, ahead))

    def forward(j):
        columns = pl.ds(j * PIECE, PIECE)
        for device, target, start in onward:
            links.start(
                target.at[pl.ds(start, depth), columns],
                target.at[pl.ds(opposite, depth), columns],
                w.forward_s,
                w.forward_r.at[j],
                device,
            )

    def forwarded(j):
        columns = pl.ds(j * PIECE, PIECE)
        links.arrived(w.gate.at[pl.ds(ahead, 2 * depth), columns], w.forward_r.at[j])

    gather(0)
    gather(1)
    for load in loads[3:]:
        load.start()

    def norm(start, rows):
        place = pl.ds(start, rows)
        wide = w.normed[place, :].astype(jnp.float32)
        factor = lax.rsqrt(jnp.mean(wide * wide, axis=-1, keepdims=True) + epsilon)
        w.normed[place, :] = (wide * factor * mix_gain_ref[...]).astype(jnp.bfloat16)

    def norm_step(i, carry):
        norm(aligned(i, 8), 8)
        return carry

    def to_inner(rows):
        w.inner[rows, :] = jnp.dot(
            w.normed[rows, :], w.in_proj[...], preferred_element_type=jnp.float32
        ).astype(jnp.bfloat16)

    small_loads[0].wait()
    for k in range(PARTS):
        row_loads[k].wait()
        steps = part_rows // 8
        lax.fori_loop(k * steps, (k + 1) * steps, norm_step, 0, unroll=4)
    loads[1].wait()
    to_inner(pl.ds(0, length))
    links.arrived(w.normed.at[edge, :], w.tail_r)
    gather(2)
    norm(length, EDGE)
    to_inner(edge)
    for load in small_loads[1:]:
        load.wait()
    local_states(
        taps,
        links.s,
        w.inner,
        conv_weight_ref,
        conv_bias_ref,
        input_gate_ref,
        input_bias_ref,
        decay_gate_ref,
        decay_bias_ref,
        decay_param_ref,
        w.decays,
        w.states,
        w.ends,
    )
    for k in range(count - 1):
        links.start(w.ends, w.arrived.at[k], w.end_s, w.end_r, peers[k])
    for n in range(3, 2 * CHUNKS):
        gather(n)
    loads[2].wait()
    branch = jax.nn.gelu(
        jnp.dot(w.normed[:length, :], w.branch_proj[...], preferred_element_type=jnp.float32), approximate=True
    )
    carried = jnp.zeros((1, w.ends.shape[1]), jnp.float32)
    links.arrived(w.arrived, w.end_r)
    for k in range(count - 2, -1, -1):
        new = w.arrived[k, 0:1, :] * carried + w.arrived[k, 1:2, :]
        carried = jnp.where(links.s >= k + 1, new, carried)
    w.gated[...] = ((w.states[...] + w.decays[...] * carried) * branch).astype(jnp.bfloat16)

    def product(left_ref, right_ref, part_ref, scratch, total_ref=None):
        tile = 512
        for g in range(GROUPS):

            def step(i, carry):
                columns = pl.ds(aligned(i, tile), tile)
                value = jnp.dot(left_ref[...], right_ref[:, columns], preferred_element_type=jnp.float32)
                if total_ref is not None:
                    value = value + total_ref[:, columns]
                part_ref[:, columns] = value.astype(jnp.bfloat16)
                return carry

            steps = width // (GROUPS * tile)
            lax.fori_loop(g * steps, (g + 1) * steps, step, 0, unroll=True)
            pair_up(links, part_ref, scratch, g)

    loads[3].wait()
    product(w.gated, w.out_proj, w.part, first)
    loads[4].wait()

    def to_middle(columns, total):
        w.middle[:, columns] = (total + w.middle[:, columns].astype(jnp.float32)).astype(jnp.bfloat16)

    reduce_scatter(links, w.part, first, to_middle)

    wide = w.middle[...].astype(jnp.float32)
    factor = lax.rsqrt(jnp.mean(wide * wide, axis=-1, keepdims=True) + epsilon)
    w.chosen[...] = (wide * factor * gain_ref[...]).astype(jnp.bfloat16)
    hidden_in = w.hidden_in

    def features(p, which):
        return pl.ds(aligned(2 * lax.rem(links.y + 3 + p, 4) + which, depth), depth)

    def slot(h, r, side):
        group = links.xh if h == 0 else 1 - links.xh
        columns = pl.ds(0, half) if side is None else pl.ds(side * (half // 2), half // 2)
        return hidden_in.at[group, pl.ds(r, unit), columns]

    tokens = Gather(links, slot, unit, spread, (0, 1))
    for p in range(4):
        w.away[:, p * depth : (p + 1) * depth] = w.chosen[:, features(p, 1 - links.xh)]
    landing = hidden_in.at[links.xh, pl.ds(own, unit), :]
    links.start(w.away, landing, w.far_s, w.far_r.at[0], links.far)
    links.start(w.away, landing, w.far_s, w.far_r.at[1], links.outside)
    for p in range(4):
        hidden_in[links.xh, pl.ds(own, unit), p * depth : (p + 1) * depth] = w.chosen[:, features(p, links.xh)]
    tokens.near(0)
    tokens.send(0, 0)
    gathered(0)
    for j in range(pieces):
        forward(j)
    for i in (1, 0):
        links.arrived(slot(1, tokens.row(0, i), None), w.far_r.at[i])
        tokens.send(1, i)
    for i in (1, 0):
        tokens.relay(1, i)
    tokens.relay(0, 0)
    tokens.from_near(0)
    for i in (1, 0):
        tokens.relayed(1, i)
    others = pl.ds(aligned(1 - links.core, length // 2), length // 2)
    links.arrived(hidden_in.at[1 - links.xh, others, :], spread.pair_r.at[1])

    loads[5].wait()
    loads[6].wait()
    gathered(1)

    top = length // 2
    sides = ((links.x_up, 0), (links.x_down, 1))

    def partial(group, j):
        return jnp.concatenate(
            [
                jnp.dot(
                    hidden_in[group],
                    weights[:, j * PIECE : (j + 1) * PIECE],
                    preferred_element_type=jnp.float32,
                )
                for weights in (w.gate, w.up)
            ],
            axis=1,
        )

    def give(j):
        forwarded(j)
        w.given[j] = partial(1 - links.xh, j).astype(jnp.bfloat16)
        for device, d in sides:
            links.start(
                w.given.at[j, pl.ds(d * top, top), :],
                w.relay.at[d, j],
                w.relay_s,
                w.relay_r.at[j],
                device,
            )

    def keep(j):
        w.kept[j] = partial(links.xh, j)

    def pass_on(j):
        links.arrived(w.relay.at[:, j], w.relay_r.at[j])
        for device, d in sides:
            links.start(
                w.relay.at[d, j], w.taken.at[d, j], w.taken_s, w.taken_r.at[j], device
            )

    def take(j):
        links.arrived(w.taken.at[:, j], w.taken_r.at[j])
        for device, d in sides:
            rows = pl.ds(d * top, top)
            both = w.kept[j, rows, :] + w.taken[d, j].astype(jnp.float32)
            w.hidden[rows, j * PIECE : (j + 1) * PIECE] = (
                jax.nn.gelu(both[:, :PIECE], approximate=True) * both[:, PIECE:]
            ).astype(jnp.bfloat16)

    give(0)
    tokens.relay(0, 1)
    give(1)
    for j in range(pieces):
        pass_on(j)
        if j + 2 < pieces:
            give(j + 2)
        if j == 0:
            for i in range(2):
                tokens.relayed(0, i)
        if j == 1:
            links.arrived(hidden_in.at[links.xh, others, :], spread.pair_r.at[0])
            keep(0)
        if j > 0:
            keep(j)
        if j > 1:
            take(j - 2)

    loads[7].wait()
    early = (pieces - 2) * PIECE

    def sum_early(i, carry):
        columns = pl.ds(aligned(i, 512), 512)
        w.total[:, columns] = jnp.dot(
            w.hidden[:, :early], w.down[:early, columns], preferred_element_type=jnp.float32
        )
        return carry

    lax.fori_loop(0, width // 512, sum_early, 0, unroll=4)
    take(pieces - 2)
    take(pieces - 1)
    product(w.hidden.at[:, pl.ds(early, 2 * PIECE)], w.down.at[pl.ds(early, 2 * PIECE), :], w.part2, second, w.total)

    def to_out(columns, total):
        out_ref[pl.ds(own, unit), columns] = (
            total + w.middle[:, columns].astype(jnp.float32)
        ).astype(jnp.bfloat16)

    reduce_scatter(links, w.part2, second, to_out)

    def place(h, r, side):
        size = half if side is None else half // 2
        return out_ref.at[pl.ds(r, unit), pl.ds(h * half + (0 if side is None else side * size), size)]

    rows = Gather(links, place, unit, final, (0, 0))
    for h in range(2):
        rows.near(h)
        rows.send(h, 0)
    for h in range(2):
        rows.from_near(h)
    for i in range(2):
        for h in range(2):
            rows.relay(h, i)
    for i in range(2):
        for h in range(2):
            rows.relayed(h, i)
    links.arrived(out_ref.at[others, :], final.pair_r.at[0])

    links.sent_in_all(w.normed.at[edge, :], w.tail_s)
    links.sent_in_all(w.arrived, w.end_s)
    links.sent_in_all(w.gate, w.gather_s)
    links.sent_in_all(w.gate.at[pl.ds(0, 2 * depth), :], w.forward_s)
    links.sent_in_all(w.chosen, w.far_s)
    links.sent_in_all(w.given, w.relay_s)
    links.sent_in_all(w.relay, w.taken_s)
    links.sent_in_all(w.away, spread.near_s)
    links.sent_in_all(w.chosen, final.near_s)
    for b in (spread, final):
        links.sent_in_all(out_ref.at[pl.ds(0, 3 * unit), :], b.up_s)
        links.sent_in_all(out_ref.at[pl.ds(0, 3 * unit), :], b.down_s)
        links.sent_in_all(out_ref.at[others, :], b.pair_s)
    links.drain()


def on_device(
    residual,
    mix_gain,
    in_proj,
    branch_proj,
    conv_weight,
    conv_bias,
    input_gate,
    input_bias,
    decay_gate,
    decay_bias,
    decay_param,
    out_proj,
    mlp_gain,
    gate_proj,
    up_proj,
    down_proj,
):
    count = lax.axis_size("seq")
    length, width = residual.shape
    channels = in_proj.shape[1]
    depth, hidden_width = gate_proj.shape
    unit = length // 16
    bf, f32 = jnp.bfloat16, jnp.float32
    dma = pltpu.SemaphoreType.DMA
    outer = pl.BlockSpec(memory_space=pltpu.HBM)
    pieces = hidden_width // PIECE
    small = (
        mix_gain[None],
        conv_weight,
        conv_bias[None],
        input_gate,
        input_bias[None],
        decay_gate,
        decay_bias[None],
        decay_param[None],
        mlp_gain[None],
    )
    scratch = dict(
        small=tuple(pltpu.VMEM(array.shape, array.dtype) for array in small),
        small_load=dma((len(small),)),
        normed=pltpu.VMEM((length + EDGE, width), bf),
        in_proj=pltpu.VMEM(in_proj.shape, bf),
        branch_proj=pltpu.VMEM(branch_proj.shape, bf),
        inner=pltpu.VMEM((length + EDGE, channels), bf),
        out_proj=pltpu.VMEM(out_proj.shape, bf),
        middle=pltpu.VMEM((unit, width), bf),
        chosen=pltpu.VMEM((unit, width), bf),
        away=pltpu.VMEM((unit, width // 2), bf),
        gate=pltpu.VMEM((4 * depth, hidden_width), bf),
        up=pltpu.VMEM((4 * depth, hidden_width), bf),
        down=pltpu.VMEM(down_proj.shape, bf),
        hidden_in=pltpu.VMEM((2, length, width // 2), bf),
        given=pltpu.VMEM((pieces, length, 2 * PIECE), bf),
        kept=pltpu.VMEM((pieces, length, 2 * PIECE), f32),
        relay=pltpu.VMEM((2, pieces, length // 2, 2 * PIECE), bf),
        taken=pltpu.VMEM((2, pieces, length // 2, 2 * PIECE), bf),
        hidden=pltpu.VMEM((length, hidden_width), bf),
        total=pltpu.VMEM((length, width), f32),
        part=pltpu.VMEM((length, width), bf),
        part2=pltpu.VMEM((length, width), bf),
        gated=pltpu.VMEM((length, channels), bf),
        decays=pltpu.VMEM((length, channels), f32),
        states=pltpu.VMEM((length, channels), f32),
        ends=pltpu.VMEM((8, channels), f32),
        arrived=pltpu.VMEM((count - 1, 8, channels), f32),
        tail_s=dma,
        tail_r=dma,
        end_s=dma,
        end_r=dma,
        load=dma((8,)),
        row_load=dma((PARTS,)),
        edge=pltpu.VMEM((EDGE, width), bf),
        gather_s=dma,
        gather_r=dma((2, 2)),
        forward_s=dma,
        forward_r=dma((pieces,)),
        far_s=dma,
        far_r=dma((2,)),
        relay_s=dma,
        relay_r=dma((pieces,)),
        taken_s=dma,
        taken_r=dma((pieces,)),
    )
    return pl.pallas_call(
        functools.partial(layer_kernel, count, conv_weight.shape[0]),
        out_shape=jax.ShapeDtypeStruct((length, width), bf),
        in_specs=[outer] * 16,
        out_specs=pl.BlockSpec(memory_space=pltpu.VMEM),
        scratch_shapes=(
            scratch,
            scatter_scratch(length, width),
            scatter_scratch(length, width),
            gather_scratch(2),
            gather_scratch(1),
        ),
        compiler_params=pltpu.CompilerParams(
            collective_id=0, has_side_effects=True, vmem_limit_bytes=GRANT
        ),
    )(
        *(
            pltpu.with_memory_space_constraint(array, pltpu.HBM)
            for array in (
                *small,
                residual,
                in_proj,
                branch_proj,
                out_proj,
                gate_proj,
                up_proj,
                down_proj,
            )
        )
    )


def solution(mesh):
    in_specs = (
        P("seq", None),
        P(),
        P(None, "tp"),
        P(None, "tp"),
        P(None, "tp"),
        P("tp"),
        P("tp", None, None),
        P("tp"),
        P("tp", None, None),
        P("tp"),
        P("tp"),
        P("tp", None),
        P(),
        P("seq", "tp"),
        P("seq", "tp"),
        P("tp", None),
    )
    out_specs = P("seq", None)
    return jax.shard_map(
        on_device, mesh=mesh, in_specs=in_specs, out_specs=out_specs, check_vma=False
    )
```
